256 devices in a mesh: node: 8 (over x, core), space: 32 (over y, z).
Axes of the slice: x: 4, y: 4, z: 8, core: 2. Of those that a mesh axis runs over, the one named last changes fastest.
Arguments:
- initial: float32 [128, 256, 256], P('space'), may hold values from -1 to 1
- kappa: float32 [128, 256, 256], P('space'), may hold values from 0.3 to 3
Outputs:
- sections: float32 [8, 128, 256, 256], P('node', 'space')
The draws below stay inside these ranges and needn't reach their ends.
All inputs are finite; a program needn't handle non-finite values.
Results may differ from the reference program's by a relative error of at most 0.0002.
Values sent between devices are 32-bit elements; how exact they have to be, the bound alone decides.
A program may use at most 192 MiB of HBM per device.

```python
import math
import jax
import jax.numpy as jnp
from jax import lax

M = 8
NXY = 256
NZ = 128
SWEEPS = 2
VCYCLES = 2
SMOOTH = 2
LEVELS = 3
COARSE = 8


def level_of(own_key, shape, cuts, low, largest):
    gain = 1.0
    for axis_at, shards_of in cuts:
        heights = jax.random.uniform(jax.random.fold_in(jax.random.fold_in(own_key, 6), axis_at), (shards_of,), jnp.float32, low / len(cuts), largest / len(cuts))
        gain = gain * jnp.repeat(jnp.exp(heights), shape[axis_at] // shards_of).reshape((-1,) + (1,) * (len(shape) - 1 - axis_at))
    return gain


def setup_inputs(seed: int = 0) -> dict:
    splits = jax.random.split(jax.random.key(seed), 3)
    initial = jnp.clip(jax.random.uniform(splits[0], (NZ, NXY, NXY), jnp.float32, -1.0, 1.0) * level_of(splits[0], (NZ, NXY, NXY), ((0, 32),), -0.4, 0.0), -1.0, 1.0)
    kappa = jnp.clip(jnp.exp(math.log(3.0) - 2.3025851 * jax.random.uniform(splits[1], (NZ, NXY, NXY), jnp.float32) ** level_of(splits[1], (NZ, NXY, NXY), ((0, 32),), -0.2, 0.2)), 0.3, 3.0)
    return {"initial": initial, "kappa": kappa}


DIFFUSE = 2.0
REACT = 0.5
OMEGA = 0.8


def radau_gap(count, where):
    previous = 1.0
    current = where
    for degree in range(1, count):
        following = ((2 * degree + 1) * where * current - degree * previous) / (degree + 1)
        previous = current
        current = following
    return current - previous


def radau_table(count):
    zeros_found = []
    grid_count = 4096
    lower = -1.0
    value_low = radau_gap(count, lower)
    for place in range(1, grid_count):
        upper = -1.0 + 2.0 * place / grid_count
        value_up = radau_gap(count, upper)
        if value_low * value_up < 0.0:
            left_end = lower
            right_end = upper
            left_value = value_low
            for halving in range(100):
                middle = 0.5 * (left_end + right_end)
                middle_value = radau_gap(count, middle)
                if left_value * middle_value <= 0.0:
                    right_end = middle
                else:
                    left_end = middle
                    left_value = middle_value
            zeros_found.append(0.5 * (left_end + right_end))
        lower = upper
        value_low = value_up
    zeros_found.append(1.0)
    abscissa = [(value + 1.0) / 2.0 for value in zeros_found]
    table_rows = []
    for outer in range(count):
        table_rows.append([0.0] * count)
    for column in range(count):
        factor = [1.0]
        scale = 1.0
        for other in range(count):
            if other != column:
                widened = [0.0] * (len(factor) + 1)
                for power in range(len(factor)):
                    widened[power + 1] = widened[power + 1] + factor[power]
                    widened[power] = widened[power] - abscissa[other] * factor[power]
                factor = widened
                scale = scale * (abscissa[column] - abscissa[other])
        for outer in range(count):
            upto = abscissa[outer]
            accum = 0.0
            for power in range(len(factor)):
                accum = accum + factor[power] * upto ** (power + 1) / (power + 1)
            table_rows[outer][column] = accum / scale
    return abscissa, table_rows


def laplace(field):
    total = jnp.roll(field, -1, 1) + jnp.roll(field, 1, 1)
    total = total + jnp.roll(field, 1, 2) + jnp.roll(field, -1, 2)
    total = total + jnp.roll(field, 1, 3) + jnp.roll(field, -1, 3)
    return total - 6.0 * field


def smooth(field, source, shift):
    applied = field - shift * laplace(field)
    return field + OMEGA * (source - applied) / (1.0 + 6.0 * shift)


def restrict(field):
    a, b, c, d = field.shape
    return field.reshape(a, b // 2, 2, c // 2, 2, d // 2, 2).mean(axis=(2, 4, 6))


def prolong(field):
    return jnp.repeat(jnp.repeat(jnp.repeat(field, 2, 1), 2, 2), 2, 3)


def vcycle(level, field, source, shift):
    if level == LEVELS - 1:
        field = jnp.zeros_like(source)
        for sweep in range(COARSE):
            field = smooth(field, source, shift)
        return field
    if field is None:
        field = jnp.zeros_like(source)
    for sweep in range(SMOOTH):
        field = smooth(field, source, shift)
    remain = source - (field - shift * laplace(field))
    coarse_part = vcycle(level + 1, None, restrict(remain), shift / 4.0)
    field = field + prolong(coarse_part)
    for sweep in range(SMOOTH):
        field = smooth(field, source, shift)
    return field


def reference(initial, kappa):
    abscissa, table_rows = radau_table(M)
    quadrature = jnp.asarray(table_rows, jnp.float32)
    shift = jnp.asarray([DIFFUSE * value for value in abscissa], jnp.float32).reshape(M, 1, 1, 1)
    sections = jnp.broadcast_to(initial, (M,) + initial.shape).astype(jnp.float32)
    for sweep in range(SWEEPS):
        lap = laplace(sections)
        force = DIFFUSE * lap + REACT * kappa * (sections - sections * sections * sections)
        integral = jnp.einsum("mj,jzyx->mzyx", quadrature, force, precision=lax.Precision.HIGHEST)
        right = initial + integral - shift * lap
        for cycle in range(VCYCLES):
            sections = vcycle(0, sections, right, shift)
    return sections
```

```python
import functools

import jax
import jax.numpy as jnp
import numpy as np
from jax import lax
from jax.experimental import pallas as pl
from jax.experimental.pallas import tpu as pltpu
from jax.sharding import PartitionSpec as P

SWEEPS = 2
VCYCLES = 2
COARSE = 8
DIFFUSE = 2.0
REACT = 0.5
OMEGA = 0.8
MESH = pl.DeviceIdType.MESH
HIGH = lax.Precision.HIGHEST

NY = 4
NZ = 8
NX = 4
DIRS = [(a, b) for a in (-1, 0, 1) for b in (-1, 0, 1) if (a, b) != (0, 0)]


def radau_gap(count, where):
    previous = 1.0
    current = where
    for degree in range(1, count):
        following = ((2 * degree + 1) * where * current - degree * previous) / (degree + 1)
        previous = current
        current = following
    return current - previous


def radau_table(count):
    zeros_found = []
    grid_count = 4096
    lower = -1.0
    value_low = radau_gap(count, lower)
    for place in range(1, grid_count):
        upper = -1.0 + 2.0 * place / grid_count
        value_up = radau_gap(count, upper)
        if value_low * value_up < 0.0:
            left_end = lower
            right_end = upper
            left_value = value_low
            for halving in range(100):
                middle = 0.5 * (left_end + right_end)
                middle_value = radau_gap(count, middle)
                if left_value * middle_value <= 0.0:
                    right_end = middle
                else:
                    left_end = middle
                    left_value = middle_value
            zeros_found.append(0.5 * (left_end + right_end))
        lower = upper
        value_low = value_up
    zeros_found.append(1.0)
    abscissa = [(value + 1.0) / 2.0 for value in zeros_found]
    table_rows = []
    for outer in range(count):
        table_rows.append([0.0] * count)
    for column in range(count):
        factor = [1.0]
        scale = 1.0
        for other in range(count):
            if other != column:
                widened = [0.0] * (len(factor) + 1)
                for power in range(len(factor)):
                    widened[power + 1] = widened[power + 1] + factor[power]
                    widened[power] = widened[power] - abscissa[other] * factor[power]
                factor = widened
                scale = scale * (abscissa[column] - abscissa[other])
        for outer in range(count):
            upto = abscissa[outer]
            accum = 0.0
            for power in range(len(factor)):
                accum = accum + factor[power] * upto ** (power + 1) / (power + 1)
            table_rows[outer][column] = accum / scale
    return (abscissa, table_rows)


def coefficients(count):
    abscissa, table_rows = radau_table(count)
    rows = []
    for m in range(count):
        shift = DIFFUSE * abscissa[m]
        row = list(table_rows[m]) + [shift, sum(table_rows[m])]
        for level in range(3):
            s = shift / 4.0**level
            a = OMEGA / (1.0 + 6.0 * s)
            row += [a, a * s, 1.0 + 6.0 * s, s]
        rows.append(row + [0.0] * (24 - len(row)))
    return np.asarray(rows, np.float32)


def sides(c):
    r, l = c.shape
    total = pltpu.roll(c, 1, 0) + pltpu.roll(c, r - 1, 0)
    return total + (pltpu.roll(c, 1, 1) + pltpu.roll(c, l - 1, 1))


def sweep_planes(src, first, count, parts, use):
    each = count // parts

    def part(i, _):
        start = first + i * each
        before = src[start - 1]
        here = src[start]
        for k in range(each):
            p = start + k
            after = src[p + 1]
            use(p, here, before + after + sides(here))
            before, here = here, after
        return 0

    if parts == 1:
        part(0, 0)
    else:
        lax.fori_loop(0, parts, part, 0)


def smooth(src, dst, f, a, b, first, count, parts):
    def use(p, here, total):
        dst[p] = (1.0 - OMEGA) * here + (a * f[p] + b * total)

    sweep_planes(src, first, count, parts, use)


def kernel(
    co, initial, kappa, pick0, pick1, back0, back1, out,
    uk, a0, b0, f0, la, kx, fg, rs, st, w0, xw,
    a1, b1, f1, rs1, st1, w1, f2, va, vb,
    in_s, in_r, xi, xq, halo_s, halo_r, out_s, out_r,
):
    node = lax.axis_index("node")
    space = lax.axis_index("space")
    x, core = node // 2, lax.rem(node, 2)
    y, z = space // NZ, lax.rem(space, NZ)
    n, m = NZ * 4, a0.shape[1] - 8

    def at(dx=0, dc=0, dy=0, dz=0):
        nx = lax.rem(x + dx + NX, NX)
        nc = lax.rem(core + dc, 2)
        ny = lax.rem(y + dy + NY, NY)
        nz = lax.rem(z + dz + NZ, NZ)
        return (nx * 2 + nc, ny * NZ + nz)

    peers = [at(dz=d) for d in range(1, NZ)]
    peers += [at(dy=a, dz=b) for a in (-1, 1) for b in (-1, 0, 1)]
    peers += [at(dx=1), at(dx=-1), at(dc=1)]
    barrier = pltpu.get_barrier_semaphore()
    for peer in peers:
        pl.semaphore_signal(barrier, inc=1, device_id=peer, device_id_type=MESH)
    pl.semaphore_wait(barrier, len(peers))

    def remote(src, dst, send, recv, device):
        return pltpu.make_async_remote_copy(
            src_ref=src, dst_ref=dst, send_sem=send, recv_sem=recv, device_id=device, device_id_type=MESH
        )

    def exchange(kind, src, dst, origin, planes, rows, width):
        total = src.shape[1]

        def span(step, size, start, wrap):
            if step == 0:
                return pl.ds(start, size), pl.ds(start, size)
            if step < 0:
                return pl.ds(start, width), pl.ds(start + size, width)
            return pl.ds(start + size - width, width), pl.ds(wrap, width)

        copies = []
        for d, (a, b) in enumerate(DIRS):
            ps, pd = span(a, planes, origin, origin - width)
            qs, qd = span(b, rows, 0, total - width)
            copies.append(
                remote(src.at[ps, qs], dst.at[pd, qd], halo_s.at[kind, d], halo_r.at[kind, d], at(dy=a, dz=b))
            )
        for copy in copies:
            copy.start()
        return copies

    def finish(copies):
        for copy in copies:
            copy.wait_recv()
        for copy in copies:
            copy.wait_send()

    def xgather(sem, piece, both, order, ready, done):
        own = {}
        for q in order:
            ready(q)
            own[q] = [
                remote(piece(x, q), piece(x, q), sem.at[0, q], sem.at[1, q], at(dx=1)),
                remote(piece(x, q), piece(x, q), sem.at[2, q], sem.at[3, q], at(dx=-1)),
            ]
            for copy in own[q]:
                copy.start()
        left, right = lax.rem(x + NX - 1, NX), lax.rem(x + 1, NX)
        passed, cores = {}, {}
        for q in order:
            own[q][0].wait_recv()
            if q % 2 == 0:
                passed[q] = remote(piece(left, q), piece(left, q), sem.at[4, q], sem.at[5, q], at(dx=1))
                passed[q].start()
            own[q][1].wait_recv()
            if q % 2 == 1:
                passed[q] = remote(piece(right, q), piece(right, q), sem.at[4, q], sem.at[5, q], at(dx=-1))
                passed[q].start()
        for q in order:
            passed[q].wait_recv()
            cores[q] = remote(both(q), both(q), sem.at[6, q], sem.at[7, q], at(dc=1))
            cores[q].start()
        for q in order:
            cores[q].wait_recv()
            done(q)
        for q in order:
            own[q][0].wait_send()
            own[q][1].wait_send()
            passed[q].wait_send()
            cores[q].wait_send()

    part = m // NX

    def fetched(ref, d):
        to = lax.rem(z + d, NZ)
        src = ref.at[:, pl.ds(pl.multiple_of(to * m + x * part, part), part), :]
        dst = uk.at[core, pl.ds(4 * z, 4), pl.ds(pl.multiple_of(x * part, part), part), :]
        if d == 0:
            return pltpu.make_async_copy(src, dst, in_s.at[0])
        return remote(src, dst, in_s.at[d], in_r.at[d], at(dz=d))

    for which, ref in ((0, initial), (1, kappa)):

        @pl.when(core == which)
        def _():
            for d in range(NZ):
                fetched(ref, d).start()

    def in_piece(xs, d):
        come = lax.rem(z + NZ - d, NZ)
        return uk.at[core, pl.ds(4 * come, 4), pl.ds(pl.multiple_of(xs * part, part), part), :]

    def in_both(d):
        come = lax.rem(z + NZ - d, NZ)
        return uk.at[core, pl.ds(4 * come, 4)]

    def in_ready(d):
        if d == 0:
            fetched(initial, 0).wait()
        else:
            fetched(initial, d).wait_recv()

    xgather(xi, in_piece, in_both, (0, 1, 7, 2, 6, 3, 5, 4), in_ready, lambda q: None)
    for d in range(1, NZ):
        fetched(initial, d).wait_send()

    def fill(i, _):
        for k in range(4):
            a0[4 + i * 4 + k, pl.ds(0, m)] = uk[0, i * 4 + k]
            kx[4 + i * 4 + k, pl.ds(0, m)] = uk[1, i * 4 + k]
        return 0

    lax.fori_loop(0, n // 4, fill, 0)

    def land():
        for p in list(range(4)) + list(range(n + 4, n + 8)):
            a0[p] = la[p]

        def rows(i, _):
            for k in range(8):
                a0[4 + i * 8 + k, pl.ds(m, 8)] = la[4 + i * 8 + k, pl.ds(m, 8)]
            return 0

        lax.fori_loop(0, n // 8, rows, 0)

    copies = exchange(0, a0, la, 4, n, m, 4) + exchange(4, kx, kx, 4, n, m, 4)
    finish(copies)
    land()

    shift, rowsum = co[8], co[9]

    def first_right(p, here, total):
        lap = total - 6.0 * here
        force = DIFFUSE * lap + REACT * kx[p] * (here - here * here * here)
        f0[p] = here + (rowsum * force - shift * lap)

    sweep_planes(a0, 1, n + 6, 2, first_right)

    def second_right():
        def use(p, here, total):
            own, start = here[:m], p - 4
            lap = total[:m] - 6.0 * own
            force = DIFFUSE * lap + REACT * uk[1, start] * (own - own * own * own)
            fg[core, start // 4, x, lax.rem(start, 4)] = force
            f0[p, pl.ds(0, m)] = uk[0, start] - shift * lap

        sweep_planes(a0, 4, n, 4, use)

        def done(q):
            for k in range(4):
                total = f0[4 + 4 * q + k, pl.ds(0, m)]
                for j in range(2 * NX):
                    total = total + co[j] * fg[j % 2, q, j // 2, k]
                f0[4 + 4 * q + k, pl.ds(0, m)] = total

        xgather(xq, lambda xs, q: fg.at[core, q, xs], lambda q: fg.at[core, q], tuple(range(8)), lambda q: None, done)
        finish(exchange(4, f0, f0, 4, n, m, 4))

    def cycle():
        smooth(a0, b0, f0, co[10], co[11], 1, n + 6, 2)
        smooth(b0, a0, f0, co[10], co[11], 2, n + 4, 2)
        held = []

        def rest0(p, here, total):
            held.append((f0[p] - co[12] * here + co[13] * total)[:m])
            if len(held) == 2:
                i = (p - 5) // 2
                pair = held[0] + held[1]
                rs[0, i], rs[1, i] = pair[:, :128], pair[:, 128:]
                held.clear()

        sweep_planes(a0, 4, n, 2, rest0)

        def pairs0(i, _):
            for k in range(4):
                for h in range(2):
                    cut = pl.ds(128 * h, 128)
                    st[4 * i + k, :, cut] = (
                        rs[h, 4 * i + k, pl.ds(0, m // 2, stride=2)] + rs[h, 4 * i + k, pl.ds(1, m // 2, stride=2)]
                    )
            return 0

        lax.fori_loop(0, n // 8, pairs0, 0)
        coarse = jnp.dot(
            st[...].reshape(n * m // 4, 256), pick0[...], precision=HIGH, preferred_element_type=jnp.float32
        )
        f1[pl.ds(4, n // 2), pl.ds(0, m // 2)] = coarse.reshape(n // 2, m // 2, 128)
        finish(exchange(1, f1, f1, 4, n // 2, m // 2, 2))

        for p in range(2, n // 2 + 6):
            b1[p] = co[14] * f1[p]
        smooth(b1, a1, f1, co[14], co[15], 3, n // 2 + 2, 1)

        def rest1(p, here, total):
            held.append((f1[p] - co[16] * here + co[17] * total)[: m // 2])
            if len(held) == 2:
                rs1[(p - 5) // 2] = held[0] + held[1]
                held.clear()

        sweep_planes(a1, 4, n // 2, 1, rest1)
        for i in range(n // 4):
            st1[i] = rs1[i, pl.ds(0, m // 4, stride=2)] + rs1[i, pl.ds(1, m // 4, stride=2)]
        coarse = jnp.dot(
            st1[...].reshape(n * m // 16, 128), pick1[...], precision=HIGH, preferred_element_type=jnp.float32
        )
        f2[pl.ds(8, n // 4), pl.ds(0, m // 4)] = coarse.reshape(n // 4, m // 4, 128)
        finish(exchange(2, f2, f2, 8, n // 4, m // 4, 8))

        for p in range(n // 4 + 16):
            va[p] = co[18] * f2[p]
        now, later = va, vb
        for k in range(COARSE - 2, -1, -1):
            smooth(now, later, f2, co[18], co[19], 8 - k, n // 4 + 2 * k, 1)
            now, later = later, now

        fine = jnp.dot(
            now[pl.ds(8, n // 4), pl.ds(0, m // 4)].reshape(n * m // 16, 128),
            back1[...],
            precision=HIGH,
            preferred_element_type=jnp.float32,
        ).reshape(n // 4, m // 4, 128)
        for i in range(n // 4):
            w1[i, pl.ds(0, m // 4, stride=2)] = fine[i]
            w1[i, pl.ds(1, m // 4, stride=2)] = fine[i]
        for i in range(n // 4):
            add = w1[i]
            for k in range(2):
                p = 4 + 2 * i + k
                a1[p, pl.ds(0, m // 2)] = a1[p, pl.ds(0, m // 2)] + add
        finish(exchange(3, a1, a1, 4, n // 2, m // 2, 3))
        smooth(a1, b1, f1, co[14], co[15], 2, n // 2 + 4, 1)
        smooth(b1, a1, f1, co[14], co[15], 3, n // 2 + 2, 1)

        xw[...] = jnp.dot(
            a1[pl.ds(3, n // 2 + 2)].reshape((n // 2 + 2) * (m // 2 + 8), 128),
            back0[...],
            precision=HIGH,
            preferred_element_type=jnp.float32,
        ).reshape(n // 2 + 2, m // 2 + 8, 256)

        def widen(i, _):
            for k in range(3):
                g = 3 * i + k
                for h in range(2):
                    cut = pl.ds(128 * h, 128)
                    near = xw[g, pl.ds(0, m // 2 + 2), cut]
                    far = xw[g, pl.ds(m // 2 + 6, 2), cut]
                    for e in range(2):
                        w0[h, g, pl.ds(e, m // 2 + 2, stride=2)] = near
                        w0[h, g, pl.ds(m + 4 + e, 2, stride=2)] = far
                    add = w0[h, g]
                    for e in range(2):
                        a0[2 + 2 * g + e, :, cut] = a0[2 + 2 * g + e, :, cut] + add
            return 0

        lax.fori_loop(0, (n // 2 + 2) // 3, widen, 0)
        smooth(a0, b0, f0, co[10], co[11], 3, n + 2, 2)
        smooth(b0, a0, f0, co[10], co[11], 4, n, 2)

    def turn(v, _):
        @pl.when(v == VCYCLES)
        def _():
            second_right()

        cycle()

        @pl.when(v < SWEEPS * VCYCLES - 1)
        def _():
            finish(exchange(0, a0, la, 4, n, m, 4))
            land()

        return 0

    lax.fori_loop(0, SWEEPS * VCYCLES, turn, 0)

    def sent(d):
        to = lax.rem(z + d, NZ)
        src = a0.at[pl.ds(4 + 4 * to, 4), pl.ds(0, m), :]
        dst = out.at[:, pl.ds(pl.multiple_of(z * m, m), m), :]
        if d == 0:
            return pltpu.make_async_copy(src, dst, out_s.at[0])
        return remote(src, dst, out_s.at[d], out_r.at[d], at(dz=d))

    for d in (4, 3, 5, 2, 6, 1, 7, 0):
        sent(d).start()
    for d in (1, 7, 2, 6, 3, 5, 4):
        sent(d).wait_recv()
    for d in range(1, NZ):
        sent(d).wait_send()
    sent(0).wait()


def per_device(initial, kappa):
    count = lax.axis_size("node")
    assert count == 2 * NX and lax.axis_size("space") == NY * NZ
    thick, rows, cols = initial.shape
    assert thick == 4 and rows == 256 and cols == 256
    n, m = thick * NZ, rows // NZ
    co = jnp.asarray(coefficients(count))[lax.axis_index("node")]
    wide, half = np.arange(cols), np.arange(cols // 2)
    pick0 = np.where(wide[:, None] // 2 == half[None, :], 0.125, 0.0).astype(np.float32)
    pick1 = np.where(half[:, None] // 2 == half[None, :] % (cols // 4), 0.125, 0.0).astype(np.float32)
    back0 = np.where(half[:, None] == wide[None, :] // 2, 1.0, 0.0).astype(np.float32)
    back1 = np.where(half[:, None] == half[None, :] // 2, 1.0, 0.0).astype(np.float32)
    f32 = jnp.float32
    full = pltpu.VMEM((n + 8, m + 8, cols), f32)
    mid = pltpu.VMEM((n // 2 + 8, m // 2 + 8, cols // 2), f32)
    low = pltpu.VMEM((n // 4 + 16, m // 4 + 16, cols // 2), f32)
    dma = pltpu.SemaphoreType.DMA
    vmem = pl.BlockSpec(memory_space=pltpu.VMEM)
    hbm = pl.BlockSpec(memory_space=pl.ANY)
    result = pl.pallas_call(
        kernel,
        out_shape=jax.ShapeDtypeStruct((thick, rows, cols), f32),
        in_specs=[pl.BlockSpec(memory_space=pltpu.SMEM), hbm, hbm, vmem, vmem, vmem, vmem],
        out_specs=hbm,
        scratch_shapes=[
            pltpu.VMEM((2, n, m, cols), f32), full, full, full, full, full,
            pltpu.VMEM((2, 8, NX, n // 8, m, cols), f32),
            pltpu.VMEM((2, n // 2, m, cols // 2), f32), pltpu.VMEM((n // 2, m // 2, cols), f32),
            pltpu.VMEM((2, n // 2 + 2, m + 8, cols // 2), f32), pltpu.VMEM((n // 2 + 2, m // 2 + 8, cols), f32),
            mid, mid, mid,
            pltpu.VMEM((n // 4, m // 2, cols // 2), f32), pltpu.VMEM((n // 4, m // 4, cols // 2), f32),
            pltpu.VMEM((n // 4, m // 2, cols // 2), f32),
            low, low, low,
            dma((NZ,)), dma((NZ,)), dma((8, NZ)), dma((8, NZ)), dma((5, 8)), dma((5, 8)), dma((NZ,)), dma((NZ,)),
        ],
        compiler_params=pltpu.CompilerParams(collective_id=0, has_side_effects=True, vmem_limit_bytes=60 * 2**20),
    )(co, initial, kappa, jnp.asarray(pick0), jnp.asarray(pick1), jnp.asarray(back0), jnp.asarray(back1))
    return result[None]


def solution(mesh):
    slab = P("space", None, None)
    return jax.shard_map(
        per_device, mesh=mesh, in_specs=(slab, slab), out_specs=P("node", "space", None, None), check_vma=False
    )
```

```python
import functools

import jax
import jax.numpy as jnp
import numpy as np
from jax import lax
from jax.experimental import pallas as pl
from jax.experimental.pallas import tpu as pltpu
from jax.sharding import PartitionSpec as P

SWEEPS = 2
VCYCLES = 2
COARSE = 8
DIFFUSE = 2.0
REACT = 0.5
OMEGA = 0.8
MESH = pl.DeviceIdType.MESH
ROW = 24

NY = 4
NZ = 8
NX = 4
DIRS = [(a, b) for a in (-1, 0, 1) for b in (-1, 0, 1) if (a, b) != (0, 0)]


def radau_gap(count, where):
    previous = 1.0
    current = where
    for degree in range(1, count):
        following = ((2 * degree + 1) * where * current - degree * previous) / (degree + 1)
        previous = current
        current = following
    return current - previous


def radau_table(count):
    zeros_found = []
    grid_count = 4096
    lower = -1.0
    value_low = radau_gap(count, lower)
    for place in range(1, grid_count):
        upper = -1.0 + 2.0 * place / grid_count
        value_up = radau_gap(count, upper)
        if value_low * value_up < 0.0:
            left_end = lower
            right_end = upper
            left_value = value_low
            for halving in range(100):
                middle = 0.5 * (left_end + right_end)
                middle_value = radau_gap(count, middle)
                if left_value * middle_value <= 0.0:
                    right_end = middle
                else:
                    left_end = middle
                    left_value = middle_value
            zeros_found.append(0.5 * (left_end + right_end))
        lower = upper
        value_low = value_up
    zeros_found.append(1.0)
    abscissa = [(value + 1.0) / 2.0 for value in zeros_found]
    table_rows = []
    for outer in range(count):
        table_rows.append([0.0] * count)
    for column in range(count):
        factor = [1.0]
        scale = 1.0
        for other in range(count):
            if other != column:
                widened = [0.0] * (len(factor) + 1)
                for power in range(len(factor)):
                    widened[power + 1] = widened[power + 1] + factor[power]
                    widened[power] = widened[power] - abscissa[other] * factor[power]
                factor = widened
                scale = scale * (abscissa[column] - abscissa[other])
        for outer in range(count):
            upto = abscissa[outer]
            accum = 0.0
            for power in range(len(factor)):
                accum = accum + factor[power] * upto ** (power + 1) / (power + 1)
            table_rows[outer][column] = accum / scale
    return (abscissa, table_rows)


def coefficients(count):
    abscissa, table_rows = radau_table(count)
    rows = []
    for m in range(count):
        shift = DIFFUSE * abscissa[m]
        row = list(table_rows[m]) + [shift, sum(table_rows[m])]
        for level in range(3):
            s = shift / 4.0**level
            a = OMEGA / (1.0 + 6.0 * s)
            row += [a, a * s, 1.0 + 6.0 * s, s]
        rows.append(row + [0.0] * (ROW - len(row)))
    return np.asarray(rows, np.float32).reshape(-1)


def sides(c):
    r, l = c.shape
    total = pltpu.roll(c, 1, 0) + pltpu.roll(c, r - 1, 0)
    return total + (pltpu.roll(c, 1, 1) + pltpu.roll(c, l - 1, 1))


def sweep_planes(src, first, count, parts, use):
    each = count // parts

    def part(i, _):
        start = first + i * each
        before = src[start - 1]
        here = src[start]
        for k in range(each):
            p = start + k
            after = src[p + 1]
            use(p, here, before + after + sides(here))
            before, here = here, after
        return 0

    if parts == 1:
        part(0, 0)
    else:
        lax.fori_loop(0, parts, part, 0)


def smooth(src, dst, f, a, b, first, count, parts):
    def use(p, here, total):
        dst[p] = (1.0 - OMEGA) * here + (a * f[p] + b * total)

    sweep_planes(src, first, count, parts, use)


def choose(left, right):
    total = None
    for _ in range(3):
        piece = left.astype(jnp.bfloat16)
        left = left - piece.astype(jnp.float32)
        term = jnp.dot(piece, right, preferred_element_type=jnp.float32)
        total = term if total is None else total + term
    return total


def kernel(
    table, initial, kappa, out,
    uk, a0, b0, f0, la, fg, sums, come, rs, st, w0, xw,
    a1, b1, f1, rs1, st1, w1, pk, f2, va, vb, pick0, pick1, back0, back1,
    in_s, in_r, xi, xq, halo_s, halo_r, rows_s, rows_r, out_s, out_r,
):
    node = lax.axis_index("node")
    space = lax.axis_index("space")
    x, core = node // 2, lax.rem(node, 2)
    y, z = space // NZ, lax.rem(space, NZ)
    n, m = NZ * 4, a0.shape[1] - 8
    co = [table[node * ROW + i] for i in range(20)]

    def at(dx=0, dc=0, dy=0, dz=0):
        nx = lax.rem(x + dx + NX, NX)
        nc = lax.rem(core + dc, 2)
        ny = lax.rem(y + dy + NY, NY)
        nz = lax.rem(z + dz + NZ, NZ)
        return (nx * 2 + nc, ny * NZ + nz)

    peers = [at(dz=d) for d in range(1, NZ)]
    peers += [at(dy=a, dz=b) for a in (-1, 1) for b in (-1, 0, 1)]
    peers += [at(dx=1), at(dx=-1), at(dc=1)]
    barrier = pltpu.get_barrier_semaphore()
    for peer in peers:
        pl.semaphore_signal(barrier, inc=1, device_id=peer, device_id_type=MESH)
    pl.semaphore_wait(barrier, len(peers))

    def remote(src, dst, send, recv, device):
        return pltpu.make_async_remote_copy(
            src_ref=src, dst_ref=dst, send_sem=send, recv_sem=recv, device_id=device, device_id_type=MESH
        )

    def span(step, size, start, wrap, width):
        if step == 0:
            return pl.ds(start, size), pl.ds(start, size)
        if step < 0:
            return pl.ds(start, width), pl.ds(start + size, width)
        return pl.ds(start + size - width, width), pl.ds(wrap, width)

    def exchange(kind, src, dst, origin, planes, rows, total, width, wide, dirs=DIRS):
        copies = []
        for d, (a, b) in enumerate(DIRS):
            if (a, b) not in dirs:
                continue
            ps, pd = span(a, planes, origin, origin - width, width)
            qs, qd = span(b, rows, 0, total - wide, wide)
            copies.append(
                remote(src.at[ps, qs], dst.at[pd, qd], halo_s.at[kind, d], halo_r.at[kind, d], at(dy=a, dz=b))
            )
        for copy in copies:
            copy.start()
        return copies

    def finish(copies):
        for copy in copies:
            copy.wait_recv()
        for copy in copies:
            copy.wait_send()

    part = m // NX

    def fetched(ref, d):
        to = lax.rem(z + d, NZ)
        src = ref.at[:, pl.ds(pl.multiple_of(to * m + x * part, part), part), :]
        dst = uk.at[core, pl.ds(4 + 4 * z, 4), pl.ds(pl.multiple_of(x * part, part), part), :]
        if d == 0:
            return pltpu.make_async_copy(src, dst, in_s.at[0])
        return remote(src, dst, in_s.at[d], in_r.at[d], at(dz=d))

    for which, ref in ((0, initial), (1, kappa)):

        @pl.when(core == which)
        def _():
            for d in range(NZ):
                fetched(ref, d).start()

    def made(ref, test, value):
        i = lax.broadcasted_iota(jnp.int32, ref.shape, 0)
        j = lax.broadcasted_iota(jnp.int32, ref.shape, 1)
        ref[...] = jnp.where(test(i, j), value, 0.0).astype(jnp.bfloat16)

    made(pick0, lambda i, j: lax.shift_right_logical(i, 1) == j, 0.125)
    made(pick1, lambda i, j: lax.shift_right_logical(i, 1) == jnp.bitwise_and(j, 63), 0.125)
    made(back0, lambda i, j: i == lax.shift_right_logical(j, 1), 1.0)
    made(back1, lambda i, j: i == lax.shift_right_logical(j, 1), 1.0)

    def in_piece(xs, d):
        first = 4 + 4 * lax.rem(z + NZ - d, NZ)
        return uk.at[core, pl.ds(first, 4), pl.ds(pl.multiple_of(xs * part, part), part)]

    def in_both(d):
        return uk.at[core, pl.ds(4 + 4 * lax.rem(z + NZ - d, NZ), 4), pl.ds(0, m)]

    order = (0, 1, 7, 2, 6, 3, 5, 4)
    left, right = lax.rem(x + NX - 1, NX), lax.rem(x + 1, NX)
    own, passed, cores = {}, {}, {}
    for q in order:
        if q == 0:
            fetched(initial, q).wait()
        else:
            fetched(initial, q).wait_recv()
        own[q] = [
            remote(in_piece(x, q), in_piece(x, q), xi.at[0, q], xi.at[1, q], at(dx=1)),
            remote(in_piece(x, q), in_piece(x, q), xi.at[2, q], xi.at[3, q], at(dx=-1)),
        ]
        for copy in own[q]:
            copy.start()
    for q in order:
        own[q][0].wait_recv()
        if q % 2 == 0:
            passed[q] = remote(in_piece(left, q), in_piece(left, q), xi.at[4, q], xi.at[5, q], at(dx=1))
            passed[q].start()
        own[q][1].wait_recv()
        if q % 2 == 1:
            passed[q] = remote(in_piece(right, q), in_piece(right, q), xi.at[4, q], xi.at[5, q], at(dx=-1))
            passed[q].start()
    for q in order:
        passed[q].wait_recv()
        cores[q] = remote(in_both(q), in_both(q), xi.at[6, q], xi.at[7, q], at(dc=1))
        cores[q].start()
    mine = uk.at[core]
    finish(exchange(0, mine, mine, 4, n, m, m + 8, 4, 4))
    edges = [
        uk.at[core, pl.ds(0, 4)],
        uk.at[core, pl.ds(n + 4, 4)],
        uk.at[core, pl.ds(4, n), pl.ds(m, 8)],
    ]
    given = [remote(e, e, rows_s.at[0, i], rows_r.at[0, i], at(dc=1)) for i, e in enumerate(edges)]
    for copy in given:
        copy.start()
    for q in order:
        cores[q].wait_recv()
    finish(given)
    for q in order:
        own[q][0].wait_send()
        own[q][1].wait_send()
        passed[q].wait_send()
        cores[q].wait_send()
    for d in range(1, NZ):
        fetched(initial, d).wait_send()

    def fill(i, _):
        for k in range(4):
            a0[i * 4 + k] = uk[0, i * 4 + k]
        return 0

    lax.fori_loop(0, (n + 8) // 4, fill, 0)

    def land():
        for p in list(range(4)) + list(range(n + 4, n + 8)):
            a0[p] = la[p]

        def rows(i, _):
            for k in range(8):
                a0[4 + i * 8 + k, pl.ds(m, 8)] = la[4 + i * 8 + k, pl.ds(m, 8)]
            return 0

        lax.fori_loop(0, n // 8, rows, 0)

    shift, rowsum = co[8], co[9]

    def first_right(p, here, total):
        lap = total - 6.0 * here
        force = DIFFUSE * lap + REACT * uk[1, p] * (here - here * here * here)
        f0[p] = here + (rowsum * force - shift * lap)

    sweep_planes(a0, 1, n + 6, 2, first_right)

    def second_right():
        def toward(q):
            step = 1 - 2 * lax.rem(x, 2)
            return step if q < 4 else -step

        def sent_pair(q, dx):
            return remote(fg.at[0, core, q], fg.at[1, core, q], xq.at[0, q], xq.at[1, q], at(dx=dx))

        def sent_core(pair, q):
            ref = fg.at[pair, core, q]
            return remote(ref, ref, xq.at[2 + 2 * pair, q], xq.at[3 + 2 * pair, q], at(dc=1))

        def sent_cross(q):
            return remote(sums.at[q], come.at[q], xq.at[6, q], xq.at[7, q], at(dx=-toward(q)))

        def forces(i, _):
            for h in range(2):
                q = 4 * h + i

                def use(p, here, total):
                    own = here[:m]
                    lap = total[:m] - 6.0 * own
                    force = DIFFUSE * lap + REACT * uk[1, p, pl.ds(0, m)] * (own - own * own * own)
                    fg[0, core, q, p - 4 * q - 4] = force
                    f0[p, pl.ds(0, m)] = uk[0, p, pl.ds(0, m)] - shift * lap

                sweep_planes(a0, 4 + 4 * q, 4, 1, use)
                sent_pair(q, toward(4 * h)).start()
                sent_core(0, q).start()
            return 0

        lax.fori_loop(0, 4, forces, 0)

        def gathered(q):
            sent_core(0, q).wait_recv()
            sent_core(1, q).wait_recv()
            there = lax.rem(x + toward(q) + NX, NX)
            cross = lax.rem(x - toward(q) + NX, NX)
            nodes = [(e, c, 2 * (x if e == 0 else there) + c) for e in (0, 1) for c in (0, 1)]
            for k in range(4):
                forth, keep = None, f0[4 + 4 * q + k, pl.ds(0, m)]
                for e, c, j in nodes:
                    force = fg[e, c, q, k]
                    term = table[(2 * cross + core) * ROW + j] * force
                    forth = term if forth is None else forth + term
                    keep = keep + table[node * ROW + j] * force
                sums[q, k] = forth
                f0[4 + 4 * q + k, pl.ds(0, m)] = keep
            sent_cross(q).start()

        order = (0, 4, 1, 5, 2, 6, 3, 7)
        last = None
        for q in order:
            sent_pair(q, toward(q)).wait_recv()
            sent_core(1, q).start()
            if last is not None:
                gathered(last)
            last = q
        gathered(last)
        faces = []
        for q in order:
            sent_cross(q).wait_recv()
            for k in range(4):
                f0[4 + 4 * q + k, pl.ds(0, m)] = f0[4 + 4 * q + k, pl.ds(0, m)] + come[q, k]
            ps = pl.ds(4 + 4 * q, 4)
            for i, b in enumerate((-1, 1)):
                qs, qd = span(b, m, 0, m + 4, 4)
                faces.append(remote(f0.at[ps, qs], f0.at[ps, qd], rows_s.at[i, q], rows_r.at[i, q], at(dz=b)))
                faces[-1].start()
            if q in (0, 7):
                a = -1 if q == 0 else 1
                faces += exchange(4, f0, f0, 4, n, m, m + 8, 4, 4, [(a, b) for b in (-1, 0, 1)])
        finish(faces)
        for q in order:
            sent_pair(q, toward(q)).wait_send()
            sent_core(0, q).wait_send()
            sent_core(1, q).wait_send()
            sent_cross(q).wait_send()

    def cycle():
        smooth(a0, b0, f0, co[10], co[11], 1, n + 6, 2)
        smooth(b0, a0, f0, co[10], co[11], 2, n + 4, 2)
        held = []

        def rest0(p, here, total):
            held.append((f0[p] - co[12] * here + co[13] * total)[:m])
            if len(held) == 2:
                i = (p - 5) // 2
                pair = held[0] + held[1]
                rs[0, i], rs[1, i] = pair[:, :128], pair[:, 128:]
                held.clear()

        sweep_planes(a0, 4, n, 2, rest0)

        def pairs0(i, _):
            for k in range(4):
                for h in range(2):
                    cut = pl.ds(128 * h, 128)
                    st[4 * i + k, :, cut] = (
                        rs[h, 4 * i + k, pl.ds(0, m // 2, stride=2)] + rs[h, 4 * i + k, pl.ds(1, m // 2, stride=2)]
                    )
            return 0

        lax.fori_loop(0, n // 8, pairs0, 0)
        coarse = choose(st[...].reshape(n * m // 4, 256), pick0[...])
        f1[pl.ds(4, n // 2), pl.ds(0, m // 2)] = coarse.reshape(n // 2, m // 2, 128)
        finish(exchange(1, f1, f1, 4, n // 2, m // 2, m // 2 + 8, 2, 2))

        for p in range(2, n // 2 + 6):
            b1[p] = co[14] * f1[p]
        smooth(b1, a1, f1, co[14], co[15], 3, n // 2 + 2, 1)

        def rest1(p, here, total):
            held.append((f1[p] - co[16] * here + co[17] * total)[: m // 2])
            if len(held) == 2:
                rs1[(p - 5) // 2] = held[0] + held[1]
                held.clear()

        sweep_planes(a1, 4, n // 2, 1, rest1)
        for i in range(n // 4):
            st1[i] = rs1[i, pl.ds(0, m // 4, stride=2)] + rs1[i, pl.ds(1, m // 4, stride=2)]
        coarse = choose(st1[...].reshape(n * m // 16, 128), pick1[...]).reshape(n // 4, m // 4, 128)
        low = lax.broadcasted_iota(jnp.int32, (m // 4, 128), 1) < 64
        for i in range(n // 8):
            pk[4 + i, pl.ds(0, m // 4)] = jnp.where(low, coarse[2 * i], coarse[2 * i + 1])
        finish(exchange(2, pk, pk, 4, n // 8, m // 4, m // 4 + 16, 4, 8))

        low = lax.broadcasted_iota(jnp.int32, (m // 4 + 16, 128), 1) < 64
        for i in range(n // 8 + 8):
            here = pk[i]
            turned = pltpu.roll(here, 64, 1)
            for k, value in ((0, jnp.where(low, here, turned)), (1, jnp.where(low, turned, here))):
                f2[2 * i + k] = value
                va[2 * i + k] = co[18] * value
        now, later = va, vb
        for k in range(COARSE - 2, -1, -1):
            smooth(now, later, f2, co[18], co[19], 8 - k, n // 4 + 2 * k, 1)
            now, later = later, now

        fine = choose(now[pl.ds(8, n // 4), pl.ds(0, m // 4)].reshape(n * m // 16, 128), back1[...])
        fine = fine.reshape(n // 4, m // 4, 128)
        for i in range(n // 4):
            w1[i, pl.ds(0, m // 4, stride=2)] = fine[i]
            w1[i, pl.ds(1, m // 4, stride=2)] = fine[i]
        for i in range(n // 4):
            add = w1[i]
            for k in range(2):
                p = 4 + 2 * i + k
                a1[p, pl.ds(0, m // 2)] = a1[p, pl.ds(0, m // 2)] + add
        finish(exchange(3, a1, a1, 4, n // 2, m // 2, m // 2 + 8, 3, 3))
        smooth(a1, b1, f1, co[14], co[15], 2, n // 2 + 4, 1)
        smooth(b1, a1, f1, co[14], co[15], 3, n // 2 + 2, 1)

        fine = choose(a1[pl.ds(3, n // 2 + 2)].reshape((n // 2 + 2) * (m // 2 + 8), 128), back0[...])
        xw[...] = fine.reshape(n // 2 + 2, m // 2 + 8, 256)

        def widen(i, _):
            for k in range(3):
                g = 3 * i + k
                for h in range(2):
                    cut = pl.ds(128 * h, 128)
                    near = xw[g, pl.ds(0, m // 2 + 2), cut]
                    far = xw[g, pl.ds(m // 2 + 6, 2), cut]
                    for e in range(2):
                        w0[h, g, pl.ds(e, m // 2 + 2, stride=2)] = near
                        w0[h, g, pl.ds(m + 4 + e, 2, stride=2)] = far
                    add = w0[h, g]
                    for e in range(2):
                        a0[2 + 2 * g + e, :, cut] = a0[2 + 2 * g + e, :, cut] + add
            return 0

        lax.fori_loop(0, (n // 2 + 2) // 3, widen, 0)
        smooth(a0, b0, f0, co[10], co[11], 3, n + 2, 2)
        smooth(b0, a0, f0, co[10], co[11], 4, n, 2)

    def turn(v, _):
        @pl.when(v == VCYCLES)
        def _():
            second_right()

        cycle()

        @pl.when(v < SWEEPS * VCYCLES - 1)
        def _():
            finish(exchange(0, a0, la, 4, n, m, m + 8, 4, 4))
            land()

        return 0

    lax.fori_loop(0, SWEEPS * VCYCLES, turn, 0)

    def sent(d):
        to = lax.rem(z + d, NZ)
        src = a0.at[pl.ds(4 + 4 * to, 4), pl.ds(0, m), :]
        dst = out.at[:, pl.ds(pl.multiple_of(z * m, m), m), :]
        if d == 0:
            return pltpu.make_async_copy(src, dst, out_s.at[0])
        return remote(src, dst, out_s.at[d], out_r.at[d], at(dz=d))

    for d in (4, 3, 5, 2, 6, 1, 7, 0):
        sent(d).start()
    for d in (1, 7, 2, 6, 3, 5, 4):
        sent(d).wait_recv()
    for d in range(1, NZ):
        sent(d).wait_send()
    sent(0).wait()


def per_device(initial, kappa):
    count = lax.axis_size("node")
    assert count == 2 * NX and lax.axis_size("space") == NY * NZ
    thick, rows, cols = initial.shape
    assert thick == 4 and rows == 256 and cols == 256
    n, m = thick * NZ, rows // NZ
    f32 = jnp.float32
    full = pltpu.VMEM((n + 8, m + 8, cols), f32)
    mid = pltpu.VMEM((n // 2 + 8, m // 2 + 8, cols // 2), f32)
    low = pltpu.VMEM((n // 4 + 16, m // 4 + 16, cols // 2), f32)
    dma = pltpu.SemaphoreType.DMA
    chunks = pltpu.VMEM((8, n // 8, m, cols), f32)
    pick = lambda i, j: pltpu.VMEM((i, j), jnp.bfloat16)
    hbm = pl.BlockSpec(memory_space=pl.ANY)
    result = pl.pallas_call(
        kernel,
        out_shape=jax.ShapeDtypeStruct((thick, rows, cols), f32),
        in_specs=[pl.BlockSpec(memory_space=pltpu.SMEM), hbm, hbm],
        out_specs=hbm,
        scratch_shapes=[
            pltpu.VMEM((2, n + 8, m + 8, cols), f32), full, full, full, full,
            pltpu.VMEM((2, 2, 8, n // 8, m, cols), f32), chunks, chunks,
            pltpu.VMEM((2, n // 2, m, cols // 2), f32), pltpu.VMEM((n // 2, m // 2, cols), f32),
            pltpu.VMEM((2, n // 2 + 2, m + 8, cols // 2), f32), pltpu.VMEM((n // 2 + 2, m // 2 + 8, cols), f32),
            mid, mid, mid,
            pltpu.VMEM((n // 4, m // 2, cols // 2), f32), pltpu.VMEM((n // 4, m // 4, cols // 2), f32),
            pltpu.VMEM((n // 4, m // 2, cols // 2), f32),
            pltpu.VMEM((n // 8 + 8, m // 4 + 16, cols // 2), f32), low, low, low,
            pick(cols, cols // 2), pick(cols // 2, cols // 2), pick(cols // 2, cols), pick(cols // 2, cols // 2),
            dma((NZ,)), dma((NZ,)), dma((8, NZ)), dma((8, NZ)), dma((5, 8)), dma((5, 8)), dma((2, 8)), dma((2, 8)),
            dma((NZ,)), dma((NZ,)),
        ],
        compiler_params=pltpu.CompilerParams(collective_id=0, has_side_effects=True, vmem_limit_bytes=60 * 2**20),
    )(jnp.asarray(coefficients(count)), initial, kappa)
    return result[None]


def solution(mesh):
    slab = P("space", None, None)
    return jax.shard_map(
        per_device, mesh=mesh, in_specs=(slab, slab), out_specs=P("node", "space", None, None), check_vma=False
    )
```

```python
import functools

import jax
import jax.numpy as jnp
import numpy as np
from jax import lax
from jax.experimental import pallas as pl
from jax.experimental.pallas import tpu as pltpu
from jax.sharding import PartitionSpec as P

SWEEPS = 2
VCYCLES = 2
COARSE = 8
DIFFUSE = 2.0
REACT = 0.5
OMEGA = 0.8
MESH = pl.DeviceIdType.MESH
ROW = 24

NY = 4
NZ = 8
NX = 4
DIRS = [(a, b) for a in (-1, 0, 1) for b in (-1, 0, 1) if (a, b) != (0, 0)]


def radau_gap(count, where):
    previous = 1.0
    current = where
    for degree in range(1, count):
        following = ((2 * degree + 1) * where * current - degree * previous) / (degree + 1)
        previous = current
        current = following
    return current - previous


def radau_table(count):
    zeros_found = []
    grid_count = 4096
    lower = -1.0
    value_low = radau_gap(count, lower)
    for place in range(1, grid_count):
        upper = -1.0 + 2.0 * place / grid_count
        value_up = radau_gap(count, upper)
        if value_low * value_up < 0.0:
            left_end = lower
            right_end = upper
            left_value = value_low
            for halving in range(100):
                middle = 0.5 * (left_end + right_end)
                middle_value = radau_gap(count, middle)
                if left_value * middle_value <= 0.0:
                    right_end = middle
                else:
                    left_end = middle
                    left_value = middle_value
            zeros_found.append(0.5 * (left_end + right_end))
        lower = upper
        value_low = value_up
    zeros_found.append(1.0)
    abscissa = [(value + 1.0) / 2.0 for value in zeros_found]
    table_rows = []
    for outer in range(count):
        table_rows.append([0.0] * count)
    for column in range(count):
        factor = [1.0]
        scale = 1.0
        for other in range(count):
            if other != column:
                widened = [0.0] * (len(factor) + 1)
                for power in range(len(factor)):
                    widened[power + 1] = widened[power + 1] + factor[power]
                    widened[power] = widened[power] - abscissa[other] * factor[power]
                factor = widened
                scale = scale * (abscissa[column] - abscissa[other])
        for outer in range(count):
            upto = abscissa[outer]
            accum = 0.0
            for power in range(len(factor)):
                accum = accum + factor[power] * upto ** (power + 1) / (power + 1)
            table_rows[outer][column] = accum / scale
    return (abscissa, table_rows)


def coefficients(count):
    abscissa, table_rows = radau_table(count)
    rows = []
    for m in range(count):
        shift = DIFFUSE * abscissa[m]
        row = list(table_rows[m]) + [shift, sum(table_rows[m])]
        for level in range(3):
            s = shift / 4.0**level
            a = OMEGA / (1.0 + 6.0 * s)
            row += [a, a * s, 1.0 + 6.0 * s, s]
        rows.append(row + [0.0] * (ROW - len(row)))
    return np.asarray(rows, np.float32).reshape(-1)


def sides(c):
    r, l = c.shape
    total = pltpu.roll(c, 1, 0) + pltpu.roll(c, r - 1, 0)
    if l == 256:
        even, odd = c[:, :128], c[:, 128:]
        return total + jnp.concatenate([odd + pltpu.roll(odd, 1, 1), even + pltpu.roll(even, 127, 1)], axis=1)
    return total + (pltpu.roll(c, 1, 1) + pltpu.roll(c, l - 1, 1))


def sweep_planes(src, first, count, parts, use):
    each = count // parts

    def part(i, _):
        start = first + i * each
        before = src[start - 1]
        here = src[start]
        for k in range(each):
            p = start + k
            after = src[p + 1]
            use(p, here, before + after + sides(here))
            before, here = here, after
        return 0

    if parts == 1:
        part(0, 0)
    else:
        lax.fori_loop(0, parts, part, 0)


def smooth(src, dst, f, b, first, count, parts):
    def use(p, here, total):
        dst[p] = (1.0 - OMEGA) * here + (f[p] + b * total)

    sweep_planes(src, first, count, parts, use)


def choose(left, right):
    total = None
    for _ in range(3):
        piece = left.astype(jnp.bfloat16)
        left = left - piece.astype(jnp.float32)
        term = jnp.dot(piece, right, preferred_element_type=jnp.float32)
        total = term if total is None else total + term
    return total


def kernel(
    table, initial, kappa, out,
    uk, a0, b0, f0, la, fg, sums, come, ready, rs, w0,
    a1, b1, f1, rs1, st1, w1, pk, f2, va, vb, apart, joined, pick1, back1,
    in_s, in_r, xi, xq, halo_s, halo_r, rows_s, rows_r, side_s, side_r, out_s, out_r,
):
    node = lax.axis_index("node")
    space = lax.axis_index("space")
    x, core = node // 2, lax.rem(node, 2)
    y, z = space // NZ, lax.rem(space, NZ)
    n, m = NZ * 4, a0.shape[1] - 8
    co = [table[node * ROW + i] for i in range(20)]

    def at(dx=0, dc=0, dy=0, dz=0):
        nx = lax.rem(x + dx + NX, NX)
        nc = lax.rem(core + dc, 2)
        ny = lax.rem(y + dy + NY, NY)
        nz = lax.rem(z + dz + NZ, NZ)
        return (nx * 2 + nc, ny * NZ + nz)

    peers = [at(dz=d) for d in range(1, NZ)]
    peers += [at(dy=a, dz=b) for a in (-1, 1) for b in (-1, 0, 1)]
    peers += [at(dx=1), at(dx=-1), at(dc=1)]
    barrier = pltpu.get_barrier_semaphore()
    for peer in peers:
        pl.semaphore_signal(barrier, inc=1, device_id=peer, device_id_type=MESH)
    pl.semaphore_wait(barrier, len(peers))

    def remote(src, dst, send, recv, device):
        return pltpu.make_async_remote_copy(
            src_ref=src, dst_ref=dst, send_sem=send, recv_sem=recv, device_id=device, device_id_type=MESH
        )

    def span(step, size, start, wrap, width):
        if step == 0:
            return pl.ds(start, size), pl.ds(start, size)
        if step < 0:
            return pl.ds(start, width), pl.ds(start + size, width)
        return pl.ds(start + size - width, width), pl.ds(wrap, width)

    def exchange(kind, src, dst, origin, planes, rows, total, width, wide, dirs=DIRS, start=True):
        copies = []
        for d, (a, b) in enumerate(DIRS):
            if (a, b) not in dirs:
                continue
            ps, pd = span(a, planes, origin, origin - width, width)
            qs, qd = span(b, rows, 0, total - wide, wide)
            copies.append(
                remote(src.at[ps, qs], dst.at[pd, qd], halo_s.at[kind, d], halo_r.at[kind, d], at(dy=a, dz=b))
            )
        if start:
            for copy in copies:
                copy.start()
        return copies

    def finish(copies):
        for copy in copies:
            copy.wait_recv()
        for copy in copies:
            copy.wait_send()

    part = m // NX

    def fetched(ref, d):
        to = lax.rem(z + d, NZ)
        src = ref.at[:, pl.ds(pl.multiple_of(to * m + x * part, part), part), :]
        dst = uk.at[core, pl.ds(4 + 4 * z, 4), pl.ds(pl.multiple_of(x * part, part), part), :]
        if d == 0:
            return pltpu.make_async_copy(src, dst, in_s.at[0])
        return remote(src, dst, in_s.at[d], in_r.at[d], at(dz=d))

    for which, ref in ((0, initial), (1, kappa)):

        @pl.when(core == which)
        def _():
            for d in range(NZ):
                fetched(ref, d).start()

    def made(ref, test, value):
        i = lax.broadcasted_iota(jnp.int32, ref.shape, 0)
        j = lax.broadcasted_iota(jnp.int32, ref.shape, 1)
        ref[...] = jnp.where(test(i, j), value, 0.0).astype(jnp.bfloat16)

    half = m * NZ // 2
    made(apart, lambda i, j: i == jnp.where(j < half, 2 * j, 2 * (j - half) + 1), 1.0)
    made(joined, lambda i, j: j == jnp.where(i < half, 2 * i, 2 * (i - half) + 1), 1.0)
    made(pick1, lambda i, j: lax.shift_right_logical(i, 1) == jnp.bitwise_and(j, 63), 0.125)
    made(back1, lambda i, j: i == lax.shift_right_logical(j, 1), 1.0)

    def in_piece(xs, d):
        first = 4 + 4 * lax.rem(z + NZ - d, NZ)
        return uk.at[core, pl.ds(first, 4), pl.ds(pl.multiple_of(xs * part, part), part)]

    def in_both(d):
        return uk.at[core, pl.ds(4 + 4 * lax.rem(z + NZ - d, NZ), 4), pl.ds(0, m)]

    order = (0, 1, 7, 2, 6, 3, 5, 4)
    left, right = lax.rem(x + NX - 1, NX), lax.rem(x + 1, NX)
    own, passed, cores = {}, {}, {}
    for q in order:
        if q == 0:
            fetched(initial, q).wait()
        else:
            fetched(initial, q).wait_recv()
        here = in_piece(x, q)
        here[...] = choose(here[...].reshape(4 * part, 2 * half), apart[...]).reshape(4, part, 2 * half)
        own[q] = [
            remote(in_piece(x, q), in_piece(x, q), xi.at[0, q], xi.at[1, q], at(dx=1)),
            remote(in_piece(x, q), in_piece(x, q), xi.at[2, q], xi.at[3, q], at(dx=-1)),
        ]
        for copy in own[q]:
            copy.start()
    for q in order:
        own[q][0].wait_recv()
        if q % 2 == 0:
            passed[q] = remote(in_piece(left, q), in_piece(left, q), xi.at[4, q], xi.at[5, q], at(dx=1))
            passed[q].start()
        own[q][1].wait_recv()
        if q % 2 == 1:
            passed[q] = remote(in_piece(right, q), in_piece(right, q), xi.at[4, q], xi.at[5, q], at(dx=-1))
            passed[q].start()
    for q in order:
        passed[q].wait_recv()
        cores[q] = remote(in_both(q), in_both(q), xi.at[6, q], xi.at[7, q], at(dc=1))
        cores[q].start()
    mine = uk.at[core]
    finish(exchange(0, mine, mine, 4, n, m, m + 8, 4, 4))
    edges = [
        uk.at[core, pl.ds(0, 4)],
        uk.at[core, pl.ds(n + 4, 4)],
        uk.at[core, pl.ds(4, n), pl.ds(m, 8)],
    ]
    given = [remote(e, e, rows_s.at[0, i], rows_r.at[0, i], at(dc=1)) for i, e in enumerate(edges)]
    for copy in given:
        copy.start()
    for q in order:
        cores[q].wait_recv()
    finish(given)
    for q in order:
        own[q][0].wait_send()
        own[q][1].wait_send()
        passed[q].wait_send()
        cores[q].wait_send()
    for d in range(1, NZ):
        fetched(initial, d).wait_send()

    def fill(i, _):
        for k in range(4):
            a0[i * 4 + k] = uk[0, i * 4 + k]
        return 0

    lax.fori_loop(0, (n + 8) // 4, fill, 0)

    shift, rowsum = co[8], co[9]

    def first_right(p, here, total):
        lap = total - 6.0 * here
        force = DIFFUSE * lap + REACT * uk[1, p] * (here - here * here * here)
        f0[p] = co[10] * (here + (rowsum * force - shift * lap))

    sweep_planes(a0, 1, n + 6, 2, first_right)

    def second_right():
        def toward(q):
            step = 1 - 2 * lax.rem(x, 2)
            return step if q < 4 else -step

        def sent_pair(q, dx):
            return remote(fg.at[0, core, q], fg.at[1, core, q], xq.at[0, q], xq.at[1, q], at(dx=dx))

        def sent_core(pair, q):
            ref = fg.at[pair, core, q]
            return remote(ref, ref, xq.at[2 + 2 * pair, q], xq.at[3 + 2 * pair, q], at(dc=1))

        def sent_cross(q):
            return remote(sums.at[q], come.at[q], xq.at[6, q], xq.at[7, q], at(dx=-toward(q)))

        def forces(i, _):
            for h in range(2):
                q = 4 * h + i

                def use(p, here, total):
                    own = here[:m]
                    lap = total[:m] - 6.0 * own
                    force = DIFFUSE * lap + REACT * uk[1, p, pl.ds(0, m)] * (own - own * own * own)
                    fg[0, core, q, p - 4 * q - 4] = force
                    f0[p, pl.ds(0, m)] = co[10] * (uk[0, p, pl.ds(0, m)] - shift * lap)

                sweep_planes(a0, 4 + 4 * q, 4, 1, use)
                sent_pair(q, toward(4 * h)).start()
                sent_core(0, q).start()
            return 0

        lax.fori_loop(0, 4, forces, 0)

        def gathered(q):
            sent_core(0, q).wait_recv()
            sent_core(1, q).wait_recv()
            there = lax.rem(x + toward(q) + NX, NX)
            cross = lax.rem(x - toward(q) + NX, NX)
            nodes = [(e, c, 2 * (x if e == 0 else there) + c) for e in (0, 1) for c in (0, 1)]
            for k in range(4):
                forth, keep = None, f0[4 + 4 * q + k, pl.ds(0, m)]
                for e, c, j in nodes:
                    force = fg[e, c, q, k]
                    term = (table[(2 * cross + core) * ROW + j] * table[(2 * cross + core) * ROW + 10]) * force
                    forth = term if forth is None else forth + term
                    keep = keep + (table[node * ROW + j] * co[10]) * force
                sums[q, k] = forth
                f0[4 + 4 * q + k, pl.ds(0, m)] = keep
            sent_cross(q).start()

        order = (0, 4, 1, 5, 2, 6, 3, 7)
        last = None
        for q in order:
            sent_pair(q, toward(q)).wait_recv()
            sent_core(1, q).start()
            if last is not None:
                gathered(last)
            last = q
        gathered(last)
        faces = []
        for q in order:
            sent_cross(q).wait_recv()
            for k in range(4):
                f0[4 + 4 * q + k, pl.ds(0, m)] = f0[4 + 4 * q + k, pl.ds(0, m)] + come[q, k]
            ps = pl.ds(4 + 4 * q, 4)
            for i, b in enumerate((-1, 1)):
                qs, qd = span(b, m, 0, m + 4, 4)
                faces.append(remote(f0.at[ps, qs], f0.at[ps, qd], rows_s.at[i, q], rows_r.at[i, q], at(dz=b)))
                faces[-1].start()
            if q in (0, 7):
                a = -1 if q == 0 else 1
                faces += exchange(4, f0, f0, 4, n, m, m + 8, 4, 4, [(a, b) for b in (-1, 0, 1)])
        finish(faces)
        for q in order:
            sent_pair(q, toward(q)).wait_send()
            sent_core(0, q).wait_send()
            sent_core(1, q).wait_send()
            sent_cross(q).wait_send()

    def cycle(v):
        smooth(b0, a0, f0, co[11], 2, n + 4, 1)
        held = []

        def rest0(p, here, total):
            held.append((f0[p] - OMEGA * here + co[11] * total)[:m])
            if len(held) == 2:
                pair = held[0] + held[1]
                rs[(p - 5) // 2] = pair[:, :128] + pair[:, 128:]
                held.clear()

        sweep_planes(a0, 4, n, 1, rest0)
        mean = 0.125 * co[14] / co[10]
        for i in range(n // 2):
            f1[4 + i, pl.ds(0, m // 2)] = mean * (
                rs[i, pl.ds(0, m // 2, stride=2)] + rs[i, pl.ds(1, m // 2, stride=2)]
            )
        finish(exchange(1, f1, f1, 4, n // 2, m // 2, m // 2 + 8, 2, 2))

        smooth(f1, a1, f1, co[15], 3, n // 2 + 2, 1)

        def rest1(p, here, total):
            held.append((f1[p] - OMEGA * here + co[15] * total)[: m // 2])
            if len(held) == 2:
                rs1[(p - 5) // 2] = held[0] + held[1]
                held.clear()

        sweep_planes(a1, 4, n // 2, 1, rest1)
        for i in range(n // 4):
            st1[i] = (co[18] / co[14]) * (
                rs1[i, pl.ds(0, m // 4, stride=2)] + rs1[i, pl.ds(1, m // 4, stride=2)]
            )
        coarse = choose(st1[...].reshape(n * m // 16, 128), pick1[...]).reshape(n // 4, m // 4, 128)
        low = lax.broadcasted_iota(jnp.int32, (m // 4, 128), 1) < 64
        for i in range(n // 8):
            pk[4 + i, pl.ds(0, m // 4)] = jnp.where(low, coarse[2 * i], coarse[2 * i + 1])
        finish(exchange(2, pk, pk, 4, n // 8, m // 4, m // 4 + 16, 4, 8))

        low = lax.broadcasted_iota(jnp.int32, (m // 4 + 16, 128), 1) < 64
        for i in range(n // 8 + 8):
            here = pk[i]
            turned = pltpu.roll(here, 64, 1)
            for k, value in ((0, jnp.where(low, here, turned)), (1, jnp.where(low, turned, here))):
                f2[2 * i + k] = value
        now, later = f2, va
        for k in range(COARSE - 2, -1, -1):
            smooth(now, later, f2, co[19], 8 - k, n // 4 + 2 * k, 1)
            now, later = later, vb if later is va else va

        fine = choose(now[pl.ds(8, n // 4), pl.ds(0, m // 4)].reshape(n * m // 16, 128), back1[...])
        fine = fine.reshape(n // 4, m // 4, 128)
        for i in range(n // 4):
            w1[i, pl.ds(0, m // 4, stride=2)] = fine[i]
            w1[i, pl.ds(1, m // 4, stride=2)] = fine[i]
        for i in range(n // 4):
            add = w1[i]
            for k in range(2):
                p = 4 + 2 * i + k
                a1[p, pl.ds(0, m // 2)] = a1[p, pl.ds(0, m // 2)] + add
        finish(exchange(3, a1, a1, 4, n // 2, m // 2, m // 2 + 8, 3, 3))
        smooth(a1, b1, f1, co[15], 2, n // 2 + 4, 1)
        smooth(b1, a1, f1, co[15], 3, n // 2 + 2, 1)

        for g in range(n // 2 + 2):
            near = a1[3 + g, pl.ds(0, m // 2 + 2)]
            far = a1[3 + g, pl.ds(m // 2 + 6, 2)]
            for e in range(2):
                w0[g, pl.ds(e, m // 2 + 2, stride=2)] = near
                w0[g, pl.ds(m + 4 + e, 2, stride=2)] = far
        for g in range(n // 2 + 2):
            add = jnp.concatenate([w0[g], w0[g]], axis=1)
            for e in range(2):
                a0[2 + 2 * g + e] = a0[2 + 2 * g + e] + add
        smooth(a0, b0, f0, co[11], 3, n + 2, 1)

        smooth(b0, a0, f0, co[11], 4, 4, 1)
        smooth(b0, a0, f0, co[11], n, 4, 1)

        @pl.when(v < SWEEPS * VCYCLES - 1)
        def _():
            for copy in plane_faces():
                copy.start()

        for h in range(2):
            smooth(b0, a0, f0, co[11], 8 + h * (n // 2 - 4), n // 2 - 4, 1)

            @pl.when(v < SWEEPS * VCYCLES - 1)
            def _():
                for copy in row_faces(h):
                    copy.start()

    def plane_faces():
        return exchange(
            0, a0, la, 4, n, m, m + 8, 4, 4, [(a, b) for a in (-1, 1) for b in (-1, 0, 1)], start=False
        )

    def row_faces(h):
        ps = pl.ds(4 + h * (n // 2), n // 2)
        faces = []
        for i, b in enumerate((-1, 1)):
            qs, qd = span(b, m, 0, m + 4, 4)
            faces.append(remote(a0.at[ps, qs], la.at[ps, qd], side_s.at[i, h], side_r.at[i, h], at(dz=b)))
        return faces

    def land_rows(h):
        for copy in row_faces(h):
            copy.wait_recv()
        for k in range(n // 2):
            p = 4 + h * (n // 2) + k
            a0[p, pl.ds(m, 8)] = la[p, pl.ds(m, 8)]

    def land_planes():
        for copy in plane_faces():
            copy.wait_recv()
        for p in list(range(4)) + list(range(n + 4, n + 8)):
            a0[p] = la[p]

    def all_sent():
        for copy in plane_faces() + row_faces(0) + row_faces(1):
            copy.wait_send()

    def turn(v, _):
        @pl.when(lax.rem(v, VCYCLES) == 0)
        def _():
            @pl.when(v > 0)
            def _():
                land_rows(0)
                land_rows(1)
                land_planes()
                second_right()
                all_sent()

            smooth(a0, b0, f0, co[11], 1, n + 6, 2)

        @pl.when(lax.rem(v, VCYCLES) != 0)
        def _():
            land_rows(0)
            smooth(a0, b0, f0, co[11], 5, n // 2 - 2, 1)
            land_rows(1)
            smooth(a0, b0, f0, co[11], n // 2 + 3, n // 2, 1)
            land_planes()
            smooth(a0, b0, f0, co[11], 1, 4, 1)
            smooth(a0, b0, f0, co[11], n + 3, 4, 1)
            all_sent()

        cycle(v)
        return 0

    lax.fori_loop(0, SWEEPS * VCYCLES, turn, 0)

    def sent(d):
        src = ready.at[d]
        dst = out.at[:, pl.ds(pl.multiple_of(z * m, m), m), :]
        if d == 0:
            return pltpu.make_async_copy(src, dst, out_s.at[0])
        return remote(src, dst, out_s.at[d], out_r.at[d], at(dz=d))

    for d in (4, 3, 5, 2, 6, 1, 7, 0):
        first = 4 + 4 * lax.rem(z + d, NZ)
        block = a0[pl.ds(first, 4), pl.ds(0, m)].reshape(4 * m, 2 * half)
        ready[d] = choose(block, joined[...]).reshape(4, m, 2 * half)
        sent(d).start()
    for d in (1, 7, 2, 6, 3, 5, 4):
        sent(d).wait_recv()
    for d in range(1, NZ):
        sent(d).wait_send()
    sent(0).wait()


def per_device(initial, kappa):
    count = lax.axis_size("node")
    assert count == 2 * NX and lax.axis_size("space") == NY * NZ
    thick, rows, cols = initial.shape
    assert thick == 4 and rows == 256 and cols == 256
    n, m = thick * NZ, rows // NZ
    f32 = jnp.float32
    full = pltpu.VMEM((n + 8, m + 8, cols), f32)
    mid = pltpu.VMEM((n // 2 + 8, m // 2 + 8, cols // 2), f32)
    low = pltpu.VMEM((n // 4 + 16, m // 4 + 16, cols // 2), f32)
    dma = pltpu.SemaphoreType.DMA
    chunks = pltpu.VMEM((8, n // 8, m, cols), f32)
    pick = lambda i, j: pltpu.VMEM((i, j), jnp.bfloat16)
    hbm = pl.BlockSpec(memory_space=pl.ANY)
    result = pl.pallas_call(
        kernel,
        out_shape=jax.ShapeDtypeStruct((thick, rows, cols), f32),
        in_specs=[pl.BlockSpec(memory_space=pltpu.SMEM), hbm, hbm],
        out_specs=hbm,
        scratch_shapes=[
            pltpu.VMEM((2, n + 8, m + 8, cols), f32), full, full, full, full,
            pltpu.VMEM((2, 2, 8, n // 8, m, cols), f32), chunks, chunks, chunks,
            pltpu.VMEM((n // 2, m, cols // 2), f32), pltpu.VMEM((n // 2 + 2, m + 8, cols // 2), f32),
            mid, mid, mid,
            pltpu.VMEM((n // 4, m // 2, cols // 2), f32), pltpu.VMEM((n // 4, m // 4, cols // 2), f32),
            pltpu.VMEM((n // 4, m // 2, cols // 2), f32),
            pltpu.VMEM((n // 8 + 8, m // 4 + 16, cols // 2), f32), low, low, low,
            pick(cols, cols), pick(cols, cols), pick(cols // 2, cols // 2), pick(cols // 2, cols // 2),
            dma((NZ,)), dma((NZ,)), dma((8, NZ)), dma((8, NZ)), dma((5, 8)), dma((5, 8)), dma((2, 8)), dma((2, 8)), dma((2, 2)), dma((2, 2)),
            dma((NZ,)), dma((NZ,)),
        ],
        compiler_params=pltpu.CompilerParams(collective_id=0, has_side_effects=True, vmem_limit_bytes=60 * 2**20),
    )(jnp.asarray(coefficients(count)), initial, kappa)
    return result[None]


def solution(mesh):
    slab = P("space", None, None)
    return jax.shard_map(
        per_device, mesh=mesh, in_specs=(slab, slab), out_specs=P("node", "space", None, None), check_vma=False
    )
```

```python
import functools

import jax
import jax.numpy as jnp
import numpy as np
from jax import lax
from jax.experimental import pallas as pl
from jax.experimental.pallas import tpu as pltpu
from jax.sharding import PartitionSpec as P

SWEEPS = 2
VCYCLES = 2
COARSE = 8
DIFFUSE = 2.0
REACT = 0.5
OMEGA = 0.8
MESH = pl.DeviceIdType.MESH
ROW = 24

NY = 4
NZ = 8
NX = 4
DIRS = [(-1, -1), (-1, 1), (1, -1), (1, 1), (-1, 0), (1, 0), (0, -1), (0, 1)]


def radau_gap(count, where):
    previous = 1.0
    current = where
    for degree in range(1, count):
        following = ((2 * degree + 1) * where * current - degree * previous) / (degree + 1)
        previous = current
        current = following
    return current - previous


def radau_table(count):
    zeros_found = []
    grid_count = 4096
    lower = -1.0
    value_low = radau_gap(count, lower)
    for place in range(1, grid_count):
        upper = -1.0 + 2.0 * place / grid_count
        value_up = radau_gap(count, upper)
        if value_low * value_up < 0.0:
            left_end = lower
            right_end = upper
            left_value = value_low
            for halving in range(100):
                middle = 0.5 * (left_end + right_end)
                middle_value = radau_gap(count, middle)
                if left_value * middle_value <= 0.0:
                    right_end = middle
                else:
                    left_end = middle
                    left_value = middle_value
            zeros_found.append(0.5 * (left_end + right_end))
        lower = upper
        value_low = value_up
    zeros_found.append(1.0)
    abscissa = [(value + 1.0) / 2.0 for value in zeros_found]
    table_rows = []
    for outer in range(count):
        table_rows.append([0.0] * count)
    for column in range(count):
        factor = [1.0]
        scale = 1.0
        for other in range(count):
            if other != column:
                widened = [0.0] * (len(factor) + 1)
                for power in range(len(factor)):
                    widened[power + 1] = widened[power + 1] + factor[power]
                    widened[power] = widened[power] - abscissa[other] * factor[power]
                factor = widened
                scale = scale * (abscissa[column] - abscissa[other])
        for outer in range(count):
            upto = abscissa[outer]
            accum = 0.0
            for power in range(len(factor)):
                accum = accum + factor[power] * upto ** (power + 1) / (power + 1)
            table_rows[outer][column] = accum / scale
    return (abscissa, table_rows)


def coefficients(count):
    abscissa, table_rows = radau_table(count)
    rows = []
    for m in range(count):
        shift = DIFFUSE * abscissa[m]
        row = list(table_rows[m]) + [shift, sum(table_rows[m])]
        for level in range(3):
            s = shift / 4.0**level
            a = OMEGA / (1.0 + 6.0 * s)
            row += [a, a * s, 1.0 + 6.0 * s, s]
        rows.append(row + [0.0] * (ROW - len(row)))
    return np.asarray(rows, np.float32).reshape(-1)


def sides(c):
    r, l = c.shape
    total = pltpu.roll(c, 1, 0) + pltpu.roll(c, r - 1, 0)
    if l == 256:
        even, odd = c[:, :128], c[:, 128:]
        return total + jnp.concatenate([odd + pltpu.roll(odd, 1, 1), even + pltpu.roll(even, 127, 1)], axis=1)
    return total + (pltpu.roll(c, 1, 1) + pltpu.roll(c, l - 1, 1))


def sweep_planes(src, first, count, parts, use):
    each = count // parts

    def part(i, _):
        start = first + i * each
        before = src[start - 1]
        here = src[start]
        for k in range(each):
            p = start + k
            after = src[p + 1]
            use(p, here, before + after + sides(here))
            before, here = here, after
        return 0

    if parts == 1:
        part(0, 0)
    else:
        lax.fori_loop(0, parts, part, 0)


def smooth(src, dst, f, b, first, count, parts):
    def use(p, here, total):
        dst[p] = (1.0 - OMEGA) * here + (f[p] + b * total)

    sweep_planes(src, first, count, parts, use)


def choose(left, right):
    total = None
    for _ in range(3):
        piece = left.astype(jnp.bfloat16)
        left = left - piece.astype(jnp.float32)
        term = jnp.dot(piece, right, preferred_element_type=jnp.float32)
        total = term if total is None else total + term
    return total


def kernel(
    numbers, initial, kappa, out,
    table, uk, a0, b0, f0, la, fg, sums, come, ready, rs, w0,
    a1, b1, f1, rs1, st1, w1, pk, f2, va, vb, apart, joined, pick1, back1,
    in_s, in_r, xi, xq, halo_s, halo_r, rows_s, rows_r, side_s, side_r, out_s, out_r, table_s,
):
    node = lax.axis_index("node")
    space = lax.axis_index("space")
    x, core = node // 2, lax.rem(node, 2)
    y, z = space // NZ, lax.rem(space, NZ)
    n, m = NZ * 4, a0.shape[1] - 8

    def at(dx=0, dc=0, dy=0, dz=0):
        nx = lax.rem(x + dx + NX, NX)
        nc = lax.rem(core + dc, 2)
        ny = lax.rem(y + dy + NY, NY)
        nz = lax.rem(z + dz + NZ, NZ)
        return (nx * 2 + nc, ny * NZ + nz)

    peers = [at(dz=d) for d in range(1, NZ)]
    peers += [at(dy=a, dz=b) for a in (-1, 1) for b in (-1, 0, 1)]
    peers += [at(dx=1), at(dx=-1), at(dc=1)]
    fetch = pltpu.make_async_copy(numbers, table, table_s.at[0])
    fetch.start()
    barrier = pltpu.get_barrier_semaphore()
    for peer in peers:
        pl.semaphore_signal(barrier, inc=1, device_id=peer, device_id_type=MESH)
    pl.semaphore_wait(barrier, len(peers))

    def remote(src, dst, send, recv, device):
        return pltpu.make_async_remote_copy(
            src_ref=src, dst_ref=dst, send_sem=send, recv_sem=recv, device_id=device, device_id_type=MESH
        )

    def span(step, size, start, wrap, width):
        if step == 0:
            return pl.ds(start, size), pl.ds(start, size)
        if step < 0:
            return pl.ds(start, width), pl.ds(start + size, width)
        return pl.ds(start + size - width, width), pl.ds(wrap, width)

    def exchange(kind, src, dst, origin, planes, rows, total, width, wide, dirs=DIRS, start=True):
        copies = []
        for d, (a, b) in enumerate(DIRS):
            if (a, b) not in dirs:
                continue
            ps, pd = span(a, planes, origin, origin - width, width)
            qs, qd = span(b, rows, 0, total - wide, wide)
            copies.append(
                remote(src.at[ps, qs], dst.at[pd, qd], halo_s.at[kind, d], halo_r.at[kind, d], at(dy=a, dz=b))
            )
        if start:
            for copy in copies:
                copy.start()
        return copies

    def finish(copies):
        for copy in copies:
            copy.wait_recv()
        for copy in copies:
            copy.wait_send()

    part = m // NX

    def fetched(ref, d):
        to = lax.rem(z + d, NZ)
        src = ref.at[:, pl.ds(pl.multiple_of(to * m + x * part, part), part), :]
        dst = uk.at[core, pl.ds(4 + 4 * z, 4), pl.ds(pl.multiple_of(x * part, part), part), :]
        if d == 0:
            return pltpu.make_async_copy(src, dst, in_s.at[0])
        return remote(src, dst, in_s.at[d], in_r.at[d], at(dz=d))

    for which, ref in ((0, initial), (1, kappa)):

        @pl.when(core == which)
        def _():
            for d in range(NZ):
                fetched(ref, d).start()

    def made(ref, test, value):
        i = lax.broadcasted_iota(jnp.int32, ref.shape, 0)
        j = lax.broadcasted_iota(jnp.int32, ref.shape, 1)
        ref[...] = jnp.where(test(i, j), value, 0.0).astype(jnp.bfloat16)

    half = m * NZ // 2
    made(apart, lambda i, j: i == jnp.where(j < half, 2 * j, 2 * (j - half) + 1), 1.0)
    made(joined, lambda i, j: j == jnp.where(i < half, 2 * i, 2 * (i - half) + 1), 1.0)
    made(pick1, lambda i, j: lax.shift_right_logical(i, 1) == jnp.bitwise_and(j, 63), 0.125)
    made(back1, lambda i, j: i == lax.shift_right_logical(j, 1), 1.0)

    def in_piece(xs, d):
        first = 4 + 4 * lax.rem(z + NZ - d, NZ)
        return uk.at[core, pl.ds(first, 4), pl.ds(pl.multiple_of(xs * part, part), part)]

    def in_both(d):
        return uk.at[core, pl.ds(4 + 4 * lax.rem(z + NZ - d, NZ), 4), pl.ds(0, m)]

    order = (0, 1, 7, 2, 6, 3, 5, 4)
    left, right = lax.rem(x + NX - 1, NX), lax.rem(x + 1, NX)
    mine = uk.at[core]
    own, passed, cores, faces = {}, {}, {}, []

    def arrived(q):
        if q == 0:
            fetched(initial, q).wait()
        else:
            fetched(initial, q).wait_recv()
        here = in_piece(x, q)
        here[...] = choose(here[...].reshape(4 * part, 2 * half), apart[...]).reshape(4, part, 2 * half)
        own[q] = [
            remote(in_piece(x, q), in_piece(x, q), xi.at[0, q], xi.at[1, q], at(dx=1)),
            remote(in_piece(x, q), in_piece(x, q), xi.at[2, q], xi.at[3, q], at(dx=-1)),
        ]
        for copy in own[q]:
            copy.start()

    def pass_on(q):
        own[q][0].wait_recv()
        if q % 2 == 0:
            passed[q] = remote(in_piece(left, q), in_piece(left, q), xi.at[4, q], xi.at[5, q], at(dx=1))
            passed[q].start()
        own[q][1].wait_recv()
        if q % 2 == 1:
            passed[q] = remote(in_piece(right, q), in_piece(right, q), xi.at[4, q], xi.at[5, q], at(dx=-1))
            passed[q].start()

    def first_faces(a, start):
        return exchange(0, mine, mine, 4, n, m, m + 8, 4, 4, [(a, b) for b in (-1, 0, 1)], start)

    def complete(q):
        passed[q].wait_recv()
        come_z = lax.rem(z + NZ - q, NZ)
        ps = pl.ds(4 + 4 * come_z, 4)
        for i, b in enumerate((-1, 1)):
            qs, qd = span(b, m, 0, m + 4, 4)
            faces.append(remote(mine.at[ps, qs], mine.at[ps, qd], rows_s.at[i, q], rows_r.at[i, q], at(dz=b)))
            faces[-1].start()
        for a, end in ((-1, 0), (1, NZ - 1)):

            @pl.when(come_z == end)
            def _():
                first_faces(a, True)

        cores[q] = remote(in_both(q), in_both(q), xi.at[6, q], xi.at[7, q], at(dc=1))
        cores[q].start()

    for i in range(NZ + 4):
        if i < NZ:
            arrived(order[i])
        if 2 <= i < NZ + 2:
            pass_on(order[i - 2])
        if 4 <= i:
            complete(order[i - 4])
    for q in order:
        cores[q].wait_recv()

    def fill(i, _):
        for k in range(4):
            a0[4 + i * 4 + k, pl.ds(0, m)] = uk[0, 4 + i * 4 + k, pl.ds(0, m)]
        return 0

    lax.fori_loop(0, n // 4, fill, 0)
    finish(faces + first_faces(-1, False) + first_faces(1, False))
    edges = [
        uk.at[core, pl.ds(0, 4)],
        uk.at[core, pl.ds(n + 4, 4)],
        uk.at[core, pl.ds(4, n), pl.ds(m, 8)],
    ]
    given = [remote(e, e, side_s.at[i // 2, i % 2], side_r.at[i // 2, i % 2], at(dc=1)) for i, e in enumerate(edges)]
    for copy in given:
        copy.start()
    for q in order:
        own[q][0].wait_send()
        own[q][1].wait_send()
        passed[q].wait_send()
        cores[q].wait_send()
    for d in range(1, NZ):
        fetched(initial, d).wait_send()
    finish(given)
    for p in list(range(4)) + list(range(n + 4, n + 8)):
        a0[p] = uk[0, p]

    def fill_rows(i, _):
        for k in range(8):
            a0[4 + i * 8 + k, pl.ds(m, 8)] = uk[0, 4 + i * 8 + k, pl.ds(m, 8)]
        return 0

    lax.fori_loop(0, n // 8, fill_rows, 0)

    fetch.wait()
    co = [table[node * ROW + i] for i in range(20)]

    shift, rowsum = co[8], co[9]

    def first_right(p, here, total):
        lap = total - 6.0 * here
        force = DIFFUSE * lap + REACT * uk[1, p] * (here - here * here * here)
        f0[p] = co[10] * (here + (rowsum * force - shift * lap))

    sweep_planes(a0, 1, n + 6, 2, first_right)

    def second_right():
        def toward(q):
            step = 1 - 2 * lax.rem(x, 2)
            return step if q < 4 else -step

        def sent_pair(q, dx):
            return remote(fg.at[0, core, q], fg.at[1, core, q], xq.at[0, q], xq.at[1, q], at(dx=dx))

        def sent_core(pair, q):
            ref = fg.at[pair, core, q]
            return remote(ref, ref, xq.at[2 + 2 * pair, q], xq.at[3 + 2 * pair, q], at(dc=1))

        def sent_cross(q):
            return remote(sums.at[q], come.at[q], xq.at[6, q], xq.at[7, q], at(dx=-toward(q)))

        def forces(i, _):
            for h in range(2):
                q = 4 * h + i

                def use(p, here, total):
                    own = here[:m]
                    lap = total[:m] - 6.0 * own
                    force = DIFFUSE * lap + REACT * uk[1, p, pl.ds(0, m)] * (own - own * own * own)
                    fg[0, core, q, p - 4 * q - 4] = force
                    f0[p, pl.ds(0, m)] = co[10] * (uk[0, p, pl.ds(0, m)] - shift * lap)

                sweep_planes(a0, 4 + 4 * q, 4, 1, use)
                sent_pair(q, toward(4 * h)).start()
                sent_core(0, q).start()
            return 0

        lax.fori_loop(0, 4, forces, 0)

        def gathered(q):
            sent_core(0, q).wait_recv()
            sent_core(1, q).wait_recv()
            there = lax.rem(x + toward(q) + NX, NX)
            cross = lax.rem(x - toward(q) + NX, NX)
            nodes = [(e, c, 2 * (x if e == 0 else there) + c) for e in (0, 1) for c in (0, 1)]
            for k in range(4):
                forth, keep = None, f0[4 + 4 * q + k, pl.ds(0, m)]
                for e, c, j in nodes:
                    force = fg[e, c, q, k]
                    term = (table[(2 * cross + core) * ROW + j] * table[(2 * cross + core) * ROW + 10]) * force
                    forth = term if forth is None else forth + term
                    keep = keep + (table[node * ROW + j] * co[10]) * force
                sums[q, k] = forth
                f0[4 + 4 * q + k, pl.ds(0, m)] = keep
            sent_cross(q).start()

        order = (0, 4, 1, 5, 2, 6, 3, 7)
        last = None
        for q in order:
            sent_pair(q, toward(q)).wait_recv()
            sent_core(1, q).start()
            if last is not None:
                gathered(last)
            last = q
        gathered(last)
        faces = []
        for q in order:
            sent_cross(q).wait_recv()
            for k in range(4):
                f0[4 + 4 * q + k, pl.ds(0, m)] = f0[4 + 4 * q + k, pl.ds(0, m)] + come[q, k]
            ps = pl.ds(4 + 4 * q, 4)
            for i, b in enumerate((-1, 1)):
                qs, qd = span(b, m, 0, m + 4, 4)
                faces.append(remote(f0.at[ps, qs], f0.at[ps, qd], rows_s.at[i, q], rows_r.at[i, q], at(dz=b)))
                faces[-1].start()
            if q in (0, 7):
                a = -1 if q == 0 else 1
                faces += exchange(4, f0, f0, 4, n, m, m + 8, 4, 4, [(a, b) for b in (-1, 0, 1)])
        finish(faces)
        for q in order:
            sent_pair(q, toward(q)).wait_send()
            sent_core(0, q).wait_send()
            sent_core(1, q).wait_send()
            sent_cross(q).wait_send()

    def cycle(v):
        smooth(b0, a0, f0, co[11], 2, n + 4, 1)
        held = []

        def rest0(p, here, total):
            held.append((f0[p] - OMEGA * here + co[11] * total)[:m])
            if len(held) == 2:
                pair = held[0] + held[1]
                rs[(p - 5) // 2] = pair[:, :128] + pair[:, 128:]
                held.clear()

        sweep_planes(a0, 4, n, 1, rest0)
        mean = 0.125 * co[14] / co[10]
        for i in range(n // 2):
            f1[4 + i, pl.ds(0, m // 2)] = mean * (
                rs[i, pl.ds(0, m // 2, stride=2)] + rs[i, pl.ds(1, m // 2, stride=2)]
            )
        finish(exchange(1, f1, f1, 4, n // 2, m // 2, m // 2 + 8, 2, 2))

        smooth(f1, a1, f1, co[15], 3, n // 2 + 2, 1)

        def rest1(p, here, total):
            held.append((f1[p] - OMEGA * here + co[15] * total)[: m // 2])
            if len(held) == 2:
                rs1[(p - 5) // 2] = held[0] + held[1]
                held.clear()

        sweep_planes(a1, 4, n // 2, 1, rest1)
        for i in range(n // 4):
            st1[i] = (co[18] / co[14]) * (
                rs1[i, pl.ds(0, m // 4, stride=2)] + rs1[i, pl.ds(1, m // 4, stride=2)]
            )
        coarse = choose(st1[...].reshape(n * m // 16, 128), pick1[...]).reshape(n // 4, m // 4, 128)
        low = lax.broadcasted_iota(jnp.int32, (m // 4, 128), 1) < 64
        for i in range(n // 8):
            pk[4 + i, pl.ds(0, m // 4)] = jnp.where(low, coarse[2 * i], coarse[2 * i + 1])
        finish(exchange(2, pk, pk, 4, n // 8, m // 4, m // 4 + 16, 4, 8))

        low = lax.broadcasted_iota(jnp.int32, (m // 4 + 16, 128), 1) < 64
        for i in range(n // 8 + 8):
            here = pk[i]
            turned = pltpu.roll(here, 64, 1)
            for k, value in ((0, jnp.where(low, here, turned)), (1, jnp.where(low, turned, here))):
                f2[2 * i + k] = value
        now, later = f2, va
        for k in range(COARSE - 2, -1, -1):
            smooth(now, later, f2, co[19], 8 - k, n // 4 + 2 * k, 1)
            now, later = later, vb if later is va else va

        fine = choose(now[pl.ds(8, n // 4), pl.ds(0, m // 4)].reshape(n * m // 16, 128), back1[...])
        fine = fine.reshape(n // 4, m // 4, 128)
        for i in range(n // 4):
            w1[i, pl.ds(0, m // 4, stride=2)] = fine[i]
            w1[i, pl.ds(1, m // 4, stride=2)] = fine[i]
        for i in range(n // 4):
            add = w1[i]
            for k in range(2):
                p = 4 + 2 * i + k
                a1[p, pl.ds(0, m // 2)] = a1[p, pl.ds(0, m // 2)] + add
        finish(exchange(3, a1, a1, 4, n // 2, m // 2, m // 2 + 8, 3, 3))
        smooth(a1, b1, f1, co[15], 2, n // 2 + 4, 1)
        smooth(b1, a1, f1, co[15], 3, n // 2 + 2, 1)

        for g in range(n // 2 + 2):
            near = a1[3 + g, pl.ds(0, m // 2 + 2)]
            far = a1[3 + g, pl.ds(m // 2 + 6, 2)]
            for e in range(2):
                w0[g, pl.ds(e, m // 2 + 2, stride=2)] = near
                w0[g, pl.ds(m + 4 + e, 2, stride=2)] = far
        for g in range(n // 2 + 2):
            add = jnp.concatenate([w0[g], w0[g]], axis=1)
            for e in range(2):
                a0[2 + 2 * g + e] = a0[2 + 2 * g + e] + add
        smooth(a0, b0, f0, co[11], 3, n + 2, 1)

        smooth(b0, a0, f0, co[11], 4, 4, 1)
        smooth(b0, a0, f0, co[11], n, 4, 1)

        @pl.when(v < SWEEPS * VCYCLES - 1)
        def _():
            for copy in plane_faces():
                copy.start()

        for h in range(2):
            smooth(b0, a0, f0, co[11], 8 + h * (n // 2 - 4), n // 2 - 4, 1)

            @pl.when(v < SWEEPS * VCYCLES - 1)
            def _():
                for copy in row_faces(h):
                    copy.start()

    def plane_faces():
        return exchange(
            0, a0, la, 4, n, m, m + 8, 4, 4, [(a, b) for a in (-1, 1) for b in (-1, 0, 1)], start=False
        )

    def row_faces(h):
        ps = pl.ds(4 + h * (n // 2), n // 2)
        faces = []
        for i, b in enumerate((-1, 1)):
            qs, qd = span(b, m, 0, m + 4, 4)
            faces.append(remote(a0.at[ps, qs], la.at[ps, qd], side_s.at[i, h], side_r.at[i, h], at(dz=b)))
        return faces

    def land_rows(h):
        for copy in row_faces(h):
            copy.wait_recv()
        for k in range(n // 2):
            p = 4 + h * (n // 2) + k
            a0[p, pl.ds(m, 8)] = la[p, pl.ds(m, 8)]

    def land_planes():
        for copy in plane_faces():
            copy.wait_recv()
        for p in list(range(4)) + list(range(n + 4, n + 8)):
            a0[p] = la[p]

    def all_sent():
        for copy in plane_faces() + row_faces(0) + row_faces(1):
            copy.wait_send()

    def turn(v, _):
        @pl.when(lax.rem(v, VCYCLES) == 0)
        def _():
            @pl.when(v > 0)
            def _():
                land_rows(0)
                land_rows(1)
                land_planes()
                second_right()
                all_sent()

            smooth(a0, b0, f0, co[11], 1, n + 6, 2)

        @pl.when(lax.rem(v, VCYCLES) != 0)
        def _():
            land_rows(0)
            smooth(a0, b0, f0, co[11], 5, n // 2 - 2, 1)
            land_rows(1)
            smooth(a0, b0, f0, co[11], n // 2 + 3, n // 2, 1)
            land_planes()
            smooth(a0, b0, f0, co[11], 1, 4, 1)
            smooth(a0, b0, f0, co[11], n + 3, 4, 1)
            all_sent()

        cycle(v)
        return 0

    lax.fori_loop(0, SWEEPS * VCYCLES, turn, 0)

    def sent(d):
        src = ready.at[d]
        dst = out.at[:, pl.ds(pl.multiple_of(z * m, m), m), :]
        if d == 0:
            return pltpu.make_async_copy(src, dst, out_s.at[0])
        return remote(src, dst, out_s.at[d], out_r.at[d], at(dz=d))

    for d in (4, 3, 5, 2, 6, 1, 7, 0):
        first = 4 + 4 * lax.rem(z + d, NZ)
        block = a0[pl.ds(first, 4), pl.ds(0, m)].reshape(4 * m, 2 * half)
        ready[d] = choose(block, joined[...]).reshape(4, m, 2 * half)
        sent(d).start()
    for d in (1, 7, 2, 6, 3, 5, 4):
        sent(d).wait_recv()
    for d in range(1, NZ):
        sent(d).wait_send()
    sent(0).wait()


def per_device(initial, kappa):
    count = lax.axis_size("node")
    assert count == 2 * NX and lax.axis_size("space") == NY * NZ
    thick, rows, cols = initial.shape
    assert thick == 4 and rows == 256 and cols == 256
    n, m = thick * NZ, rows // NZ
    f32 = jnp.float32
    full = pltpu.VMEM((n + 8, m + 8, cols), f32)
    mid = pltpu.VMEM((n // 2 + 8, m // 2 + 8, cols // 2), f32)
    low = pltpu.VMEM((n // 4 + 16, m // 4 + 16, cols // 2), f32)
    dma = pltpu.SemaphoreType.DMA
    chunks = pltpu.VMEM((8, n // 8, m, cols), f32)
    pick = lambda i, j: pltpu.VMEM((i, j), jnp.bfloat16)
    hbm = pl.BlockSpec(memory_space=pl.ANY)
    result = pl.pallas_call(
        kernel,
        out_shape=pltpu.VMEM((thick, rows, cols), f32),
        in_specs=[hbm, hbm, hbm],
        out_specs=pl.BlockSpec(memory_space=pltpu.VMEM),
        scratch_shapes=[
            pltpu.SMEM((count * ROW,), f32),
            pltpu.VMEM((2, n + 8, m + 8, cols), f32), full, full, full, full,
            pltpu.VMEM((2, 2, 8, n // 8, m, cols), f32), chunks, chunks, chunks,
            pltpu.VMEM((n // 2, m, cols // 2), f32), pltpu.VMEM((n // 2 + 2, m + 8, cols // 2), f32),
            mid, mid, mid,
            pltpu.VMEM((n // 4, m // 2, cols // 2), f32), pltpu.VMEM((n // 4, m // 4, cols // 2), f32),
            pltpu.VMEM((n // 4, m // 2, cols // 2), f32),
            pltpu.VMEM((n // 8 + 8, m // 4 + 16, cols // 2), f32), low, low, low,
            pick(cols, cols), pick(cols, cols), pick(cols // 2, cols // 2), pick(cols // 2, cols // 2),
            dma((NZ,)), dma((NZ,)), dma((8, NZ)), dma((8, NZ)), dma((5, 8)), dma((5, 8)), dma((2, 8)), dma((2, 8)), dma((2, 2)), dma((2, 2)),
            dma((NZ,)), dma((NZ,)), dma((1,)),
        ],
        compiler_params=pltpu.CompilerParams(collective_id=0, has_side_effects=True, vmem_limit_bytes=60 * 2**20),
    )(jnp.asarray(coefficients(count)), initial, kappa)
    return result[None]


def solution(mesh):
    slab = P("space", None, None)
    return jax.shard_map(
        per_device, mesh=mesh, in_specs=(slab, slab), out_specs=P("node", "space", None, None), check_vma=False
    )
```

```python
import functools

import jax
import jax.numpy as jnp
import numpy as np
from jax import lax
from jax.experimental import pallas as pl
from jax.experimental.pallas import tpu as pltpu
from jax.sharding import PartitionSpec as P

SWEEPS = 2
VCYCLES = 2
COARSE = 8
DIFFUSE = 2.0
REACT = 0.5
OMEGA = 0.8
MESH = pl.DeviceIdType.MESH
ROW = 24

NY = 4
NZ = 8
NX = 4
DIRS = [(-1, -1), (-1, 1), (1, -1), (1, 1), (-1, 0), (1, 0), (0, -1), (0, 1)]
OTHERS, ROWS = slice(0, 6), slice(6, 8)


def radau_gap(count, where):
    previous = 1.0
    current = where
    for degree in range(1, count):
        following = ((2 * degree + 1) * where * current - degree * previous) / (degree + 1)
        previous = current
        current = following
    return current - previous


def radau_table(count):
    zeros_found = []
    grid_count = 4096
    lower = -1.0
    value_low = radau_gap(count, lower)
    for place in range(1, grid_count):
        upper = -1.0 + 2.0 * place / grid_count
        value_up = radau_gap(count, upper)
        if value_low * value_up < 0.0:
            left_end = lower
            right_end = upper
            left_value = value_low
            for halving in range(100):
                middle = 0.5 * (left_end + right_end)
                middle_value = radau_gap(count, middle)
                if left_value * middle_value <= 0.0:
                    right_end = middle
                else:
                    left_end = middle
                    left_value = middle_value
            zeros_found.append(0.5 * (left_end + right_end))
        lower = upper
        value_low = value_up
    zeros_found.append(1.0)
    abscissa = [(value + 1.0) / 2.0 for value in zeros_found]
    table_rows = []
    for outer in range(count):
        table_rows.append([0.0] * count)
    for column in range(count):
        factor = [1.0]
        scale = 1.0
        for other in range(count):
            if other != column:
                widened = [0.0] * (len(factor) + 1)
                for power in range(len(factor)):
                    widened[power + 1] = widened[power + 1] + factor[power]
                    widened[power] = widened[power] - abscissa[other] * factor[power]
                factor = widened
                scale = scale * (abscissa[column] - abscissa[other])
        for outer in range(count):
            upto = abscissa[outer]
            accum = 0.0
            for power in range(len(factor)):
                accum = accum + factor[power] * upto ** (power + 1) / (power + 1)
            table_rows[outer][column] = accum / scale
    return (abscissa, table_rows)


def coefficients(count):
    abscissa, table_rows = radau_table(count)
    rows = []
    for m in range(count):
        shift = DIFFUSE * abscissa[m]
        row = list(table_rows[m]) + [shift, sum(table_rows[m])]
        for level in range(3):
            s = shift / 4.0**level
            a = OMEGA / (1.0 + 6.0 * s)
            row += [a, a * s, 1.0 + 6.0 * s, s]
        rows.append(row + [0.0] * (ROW - len(row)))
    return np.asarray(rows, np.float32).reshape(-1)


def sides(c):
    r, l = c.shape
    total = pltpu.roll(c, 1, 0) + pltpu.roll(c, r - 1, 0)
    if l == 256:
        even, odd = c[:, :128], c[:, 128:]
        return total + jnp.concatenate([odd + pltpu.roll(odd, 1, 1), even + pltpu.roll(even, 127, 1)], axis=1)
    return total + (pltpu.roll(c, 1, 1) + pltpu.roll(c, l - 1, 1))


def sweep_planes(src, first, count, parts, use):
    each = count // parts

    def part(i, _):
        start = first + i * each
        before = src[start - 1]
        here = src[start]
        for k in range(each):
            p = start + k
            after = src[p + 1]
            use(p, here, before + after + sides(here))
            before, here = here, after
        return 0

    if parts == 1:
        part(0, 0)
    else:
        lax.fori_loop(0, parts, part, 0)


def smooth(src, dst, f, b, first, count, parts):
    def use(p, here, total):
        dst[p] = (1.0 - OMEGA) * here + (f[p] + b * total)

    sweep_planes(src, first, count, parts, use)


def choose(left, right):
    total = None
    for _ in range(3):
        piece = left.astype(jnp.bfloat16)
        left = left - piece.astype(jnp.float32)
        term = jnp.dot(piece, right, preferred_element_type=jnp.float32)
        total = term if total is None else total + term
    return total


def kernel(
    numbers, initial, kappa, out,
    table, uk, a0, b0, f0, la, fg, sums, come, ready, rs, w0,
    a1, b1, f1, rs1, st1, w1, pk, f2, va, vb, apart, joined, pick1, back1,
    in_s, in_r, xi, xq, halo_s, halo_r, rows_s, rows_r, side_s, side_r, out_s, out_r, table_s,
):
    node = lax.axis_index("node")
    space = lax.axis_index("space")
    x, core = node // 2, lax.rem(node, 2)
    y, z = space // NZ, lax.rem(space, NZ)
    n, m = NZ * 4, a0.shape[1] - 8

    def at(dx=0, dc=0, dy=0, dz=0):
        nx = lax.rem(x + dx + NX, NX)
        nc = lax.rem(core + dc, 2)
        ny = lax.rem(y + dy + NY, NY)
        nz = lax.rem(z + dz + NZ, NZ)
        return (nx * 2 + nc, ny * NZ + nz)

    peers = [at(dz=d) for d in range(1, NZ)]
    peers += [at(dy=a, dz=b) for a in (-1, 1) for b in (-1, 0, 1)]
    peers += [at(dx=1), at(dx=-1), at(dc=1)]
    fetch = pltpu.make_async_copy(numbers, table, table_s.at[0])
    fetch.start()
    barrier = pltpu.get_barrier_semaphore()
    for peer in peers:
        pl.semaphore_signal(barrier, inc=1, device_id=peer, device_id_type=MESH)
    pl.semaphore_wait(barrier, len(peers))

    def remote(src, dst, send, recv, device):
        return pltpu.make_async_remote_copy(
            src_ref=src, dst_ref=dst, send_sem=send, recv_sem=recv, device_id=device, device_id_type=MESH
        )

    def span(step, size, start, wrap, width):
        if step == 0:
            return pl.ds(start, size), pl.ds(start, size)
        if step < 0:
            return pl.ds(start, width), pl.ds(start + size, width)
        return pl.ds(start + size - width, width), pl.ds(wrap, width)

    def exchange(kind, src, dst, origin, planes, rows, total, width, wide, dirs=DIRS, start=True):
        copies = []
        for d, (a, b) in enumerate(DIRS):
            if (a, b) not in dirs:
                continue
            ps, pd = span(a, planes, origin, origin - width, width)
            qs, qd = span(b, rows, 0, total - wide, wide)
            copies.append(
                remote(src.at[ps, qs], dst.at[pd, qd], halo_s.at[kind, d], halo_r.at[kind, d], at(dy=a, dz=b))
            )
        if start:
            for copy in copies:
                copy.start()
        return copies

    def finish(copies):
        for copy in copies:
            copy.wait_recv()
        for copy in copies:
            copy.wait_send()

    part = m // NX

    def fetched(ref, d):
        to = lax.rem(z + d, NZ)
        src = ref.at[:, pl.ds(pl.multiple_of(to * m + x * part, part), part), :]
        dst = uk.at[core, pl.ds(4 + 4 * z, 4), pl.ds(pl.multiple_of(x * part, part), part), :]
        if d == 0:
            return pltpu.make_async_copy(src, dst, in_s.at[0])
        return remote(src, dst, in_s.at[d], in_r.at[d], at(dz=d))

    for which, ref in ((0, initial), (1, kappa)):

        @pl.when(core == which)
        def _():
            for d in range(NZ):
                fetched(ref, d).start()

    def made(ref, test, value):
        i = lax.broadcasted_iota(jnp.int32, ref.shape, 0)
        j = lax.broadcasted_iota(jnp.int32, ref.shape, 1)
        ref[...] = jnp.where(test(i, j), value, 0.0).astype(jnp.bfloat16)

    half = m * NZ // 2
    made(apart, lambda i, j: i == jnp.where(j < half, 2 * j, 2 * (j - half) + 1), 1.0)
    made(joined, lambda i, j: j == jnp.where(i < half, 2 * i, 2 * (i - half) + 1), 1.0)
    made(pick1, lambda i, j: lax.shift_right_logical(i, 1) == jnp.bitwise_and(j, 63), 0.125)
    made(back1, lambda i, j: i == lax.shift_right_logical(j, 1), 1.0)

    def in_piece(xs, d):
        first = 4 + 4 * lax.rem(z + NZ - d, NZ)
        return uk.at[core, pl.ds(first, 4), pl.ds(pl.multiple_of(xs * part, part), part)]

    def in_both(d):
        return uk.at[core, pl.ds(4 + 4 * lax.rem(z + NZ - d, NZ), 4), pl.ds(0, m)]

    order = (0, 1, 7, 2, 6, 3, 5, 4)
    left, right = lax.rem(x + NX - 1, NX), lax.rem(x + 1, NX)
    mine = uk.at[core]
    own, passed, cores, faces = {}, {}, {}, []

    def arrived(q):
        if q == 0:
            fetched(initial, q).wait()
        else:
            fetched(initial, q).wait_recv()
        here = in_piece(x, q)
        here[...] = choose(here[...].reshape(4 * part, 2 * half), apart[...]).reshape(4, part, 2 * half)
        own[q] = [
            remote(in_piece(x, q), in_piece(x, q), xi.at[0, q], xi.at[1, q], at(dx=1)),
            remote(in_piece(x, q), in_piece(x, q), xi.at[2, q], xi.at[3, q], at(dx=-1)),
        ]
        for copy in own[q]:
            copy.start()

    def pass_on(q):
        own[q][0].wait_recv()
        if q % 2 == 0:
            passed[q] = remote(in_piece(left, q), in_piece(left, q), xi.at[4, q], xi.at[5, q], at(dx=1))
            passed[q].start()
        own[q][1].wait_recv()
        if q % 2 == 1:
            passed[q] = remote(in_piece(right, q), in_piece(right, q), xi.at[4, q], xi.at[5, q], at(dx=-1))
            passed[q].start()

    def first_faces(a, start):
        return exchange(0, mine, mine, 4, n, m, m + 8, 4, 4, [(a, b) for b in (-1, 0, 1)], start)

    def complete(q):
        passed[q].wait_recv()
        come_z = lax.rem(z + NZ - q, NZ)
        ps = pl.ds(4 + 4 * come_z, 4)
        for i, b in enumerate((-1, 1)):
            qs, qd = span(b, m, 0, m + 4, 4)
            faces.append(remote(mine.at[ps, qs], mine.at[ps, qd], rows_s.at[i, q], rows_r.at[i, q], at(dz=b)))
            faces[-1].start()
        for a, end in ((-1, 0), (1, NZ - 1)):

            @pl.when(come_z == end)
            def _():
                first_faces(a, True)

        cores[q] = remote(in_both(q), in_both(q), xi.at[6, q], xi.at[7, q], at(dc=1))
        cores[q].start()

    for i in range(NZ + 4):
        if i < NZ:
            arrived(order[i])
        if 2 <= i < NZ + 2:
            pass_on(order[i - 2])
        if 4 <= i:
            complete(order[i - 4])
    for q in order:
        cores[q].wait_recv()

    def fill(i, _):
        for k in range(4):
            a0[4 + i * 4 + k, pl.ds(0, m)] = uk[0, 4 + i * 4 + k, pl.ds(0, m)]
        return 0

    lax.fori_loop(0, n // 4, fill, 0)
    def give(i, ref):
        return remote(ref, ref, side_s.at[i // 2, i % 2], side_r.at[i // 2, i % 2], at(dc=1))

    fetch.wait()
    co = [table[node * ROW + i] for i in range(20)]
    shift, rowsum = co[8], co[9]

    def first_right(p, here, total):
        lap = total - 6.0 * here
        force = DIFFUSE * lap + REACT * uk[1, p] * (here - here * here * here)
        f0[p] = co[10] * (here + (rowsum * force - shift * lap))

    for copy in faces:
        copy.wait_recv()
    given = [give(0, mine.at[pl.ds(4, n), pl.ds(m, 8)])]
    given[0].start()
    given[0].wait_recv()

    def fill_rows(i, _):
        for k in range(8):
            a0[4 + i * 8 + k, pl.ds(m, 8)] = uk[0, 4 + i * 8 + k, pl.ds(m, 8)]
        return 0

    lax.fori_loop(0, n // 8, fill_rows, 0)
    sweep_planes(a0, 5, n - 2, 2, first_right)
    ends = first_faces(-1, False) + first_faces(1, False)
    for copy in ends:
        copy.wait_recv()
    given += [give(1, mine.at[pl.ds(0, 4)]), give(2, mine.at[pl.ds(n + 4, 4)])]
    for copy in given[1:]:
        copy.start()
    for q in order:
        own[q][0].wait_send()
        own[q][1].wait_send()
        passed[q].wait_send()
        cores[q].wait_send()
    for d in range(1, NZ):
        fetched(initial, d).wait_send()
    for copy in faces + ends:
        copy.wait_send()
    for copy in given[1:]:
        copy.wait_recv()
    for copy in given:
        copy.wait_send()
    for p in list(range(4)) + list(range(n + 4, n + 8)):
        a0[p] = uk[0, p]
    sweep_planes(a0, 1, 4, 1, first_right)
    sweep_planes(a0, n + 3, 4, 1, first_right)

    def second_right():
        def toward(q):
            step = 1 - 2 * lax.rem(x, 2)
            return step if q < 4 else -step

        def sent_pair(q, dx):
            return remote(fg.at[0, core, q], fg.at[1, core, q], xq.at[0, q], xq.at[1, q], at(dx=dx))

        def sent_core(pair, q):
            ref = fg.at[pair, core, q]
            return remote(ref, ref, xq.at[2 + 2 * pair, q], xq.at[3 + 2 * pair, q], at(dc=1))

        def sent_cross(q):
            return remote(sums.at[q], come.at[q], xq.at[6, q], xq.at[7, q], at(dx=-toward(q)))

        def forces(i, _):
            for h in range(2):
                q = 4 * h + i

                def use(p, here, total):
                    own = here[:m]
                    lap = total[:m] - 6.0 * own
                    force = DIFFUSE * lap + REACT * uk[1, p, pl.ds(0, m)] * (own - own * own * own)
                    fg[0, core, q, p - 4 * q - 4] = force
                    f0[p, pl.ds(0, m)] = co[10] * (uk[0, p, pl.ds(0, m)] - shift * lap)

                sweep_planes(a0, 4 + 4 * q, 4, 1, use)
                sent_pair(q, toward(4 * h)).start()
                sent_core(0, q).start()
            return 0

        lax.fori_loop(0, 4, forces, 0)

        def gathered(q):
            sent_core(0, q).wait_recv()
            sent_core(1, q).wait_recv()
            there = lax.rem(x + toward(q) + NX, NX)
            cross = lax.rem(x - toward(q) + NX, NX)
            nodes = [(e, c, 2 * (x if e == 0 else there) + c) for e in (0, 1) for c in (0, 1)]
            for k in range(4):
                forth, keep = None, f0[4 + 4 * q + k, pl.ds(0, m)]
                for e, c, j in nodes:
                    force = fg[e, c, q, k]
                    term = (table[(2 * cross + core) * ROW + j] * table[(2 * cross + core) * ROW + 10]) * force
                    forth = term if forth is None else forth + term
                    keep = keep + (table[node * ROW + j] * co[10]) * force
                sums[q, k] = forth
                f0[4 + 4 * q + k, pl.ds(0, m)] = keep
            sent_cross(q).start()

        order = (0, 4, 1, 5, 2, 6, 3, 7)
        last = None
        for q in order:
            sent_pair(q, toward(q)).wait_recv()
            sent_core(1, q).start()
            if last is not None:
                gathered(last)
            last = q
        gathered(last)
        faces = []
        for q in order:
            sent_cross(q).wait_recv()
            for k in range(4):
                f0[4 + 4 * q + k, pl.ds(0, m)] = f0[4 + 4 * q + k, pl.ds(0, m)] + come[q, k]
            ps = pl.ds(4 + 4 * q, 4)
            for i, b in enumerate((-1, 1)):
                qs, qd = span(b, m, 0, m + 4, 4)
                faces.append(remote(f0.at[ps, qs], f0.at[ps, qd], rows_s.at[i, q], rows_r.at[i, q], at(dz=b)))
                faces[-1].start()
            if q in (0, 7):
                a = -1 if q == 0 else 1
                faces += exchange(4, f0, f0, 4, n, m, m + 8, 4, 4, [(a, b) for b in (-1, 0, 1)])
        finish(faces)
        for q in order:
            sent_pair(q, toward(q)).wait_send()
            sent_core(0, q).wait_send()
            sent_core(1, q).wait_send()
            sent_cross(q).wait_send()

    def cycle(v):
        smooth(b0, a0, f0, co[11], 2, n + 4, 1)
        held = []

        def rest0(p, here, total):
            held.append((f0[p] - OMEGA * here + co[11] * total)[:m])
            if len(held) == 2:
                pair = held[0] + held[1]
                rs[(p - 5) // 2] = pair[:, :128] + pair[:, 128:]
                held.clear()

        sweep_planes(a0, 4, n, 1, rest0)
        mean = 0.125 * co[14] / co[10]
        for i in range(n // 2):
            f1[4 + i, pl.ds(0, m // 2)] = mean * (
                rs[i, pl.ds(0, m // 2, stride=2)] + rs[i, pl.ds(1, m // 2, stride=2)]
            )
        copies = exchange(1, f1, f1, 4, n // 2, m // 2, m // 2 + 8, 2, 2)
        for copy in copies[ROWS]:
            copy.wait_recv()

        smooth(f1, a1, f1, co[15], 5, n // 2 - 2, 1)
        for copy in copies[OTHERS]:
            copy.wait_recv()
        smooth(f1, a1, f1, co[15], 3, 2, 1)
        smooth(f1, a1, f1, co[15], n // 2 + 3, 2, 1)
        for copy in copies:
            copy.wait_send()

        def rest1(p, here, total):
            held.append((f1[p] - OMEGA * here + co[15] * total)[: m // 2])
            if len(held) == 2:
                rs1[(p - 5) // 2] = held[0] + held[1]
                held.clear()

        sweep_planes(a1, 4, n // 2, 1, rest1)
        for i in range(n // 4):
            st1[i] = (co[18] / co[14]) * (
                rs1[i, pl.ds(0, m // 4, stride=2)] + rs1[i, pl.ds(1, m // 4, stride=2)]
            )
        coarse = choose(st1[...].reshape(n * m // 16, 128), pick1[...]).reshape(n // 4, m // 4, 128)
        low = lax.broadcasted_iota(jnp.int32, (m // 4, 128), 1) < 64
        for i in range(n // 8):
            pk[4 + i, pl.ds(0, m // 4)] = jnp.where(low, coarse[2 * i], coarse[2 * i + 1])
        finish(exchange(2, pk, pk, 4, n // 8, m // 4, m // 4 + 16, 4, 8))

        low = lax.broadcasted_iota(jnp.int32, (m // 4 + 16, 128), 1) < 64
        for i in range(n // 8 + 8):
            here = pk[i]
            turned = pltpu.roll(here, 64, 1)
            for k, value in ((0, jnp.where(low, here, turned)), (1, jnp.where(low, turned, here))):
                f2[2 * i + k] = value
        now, later = f2, va
        for k in range(COARSE - 2, -1, -1):
            smooth(now, later, f2, co[19], 8 - k, n // 4 + 2 * k, 1)
            now, later = later, vb if later is va else va

        fine = choose(now[pl.ds(8, n // 4), pl.ds(0, m // 4)].reshape(n * m // 16, 128), back1[...])
        fine = fine.reshape(n // 4, m // 4, 128)
        for i in range(n // 4):
            w1[i, pl.ds(0, m // 4, stride=2)] = fine[i]
            w1[i, pl.ds(1, m // 4, stride=2)] = fine[i]
        for i in range(n // 4):
            add = w1[i]
            for k in range(2):
                p = 4 + 2 * i + k
                a1[p, pl.ds(0, m // 2)] = a1[p, pl.ds(0, m // 2)] + add
        copies = exchange(3, a1, a1, 4, n // 2, m // 2, m // 2 + 8, 3, 3)
        for copy in copies[ROWS]:
            copy.wait_recv()
        smooth(a1, b1, f1, co[15], 5, n // 2 - 2, 1)
        for copy in copies[OTHERS]:
            copy.wait_recv()
        smooth(a1, b1, f1, co[15], 2, 3, 1)
        smooth(a1, b1, f1, co[15], n // 2 + 3, 3, 1)
        for copy in copies:
            copy.wait_send()
        smooth(b1, a1, f1, co[15], 3, n // 2 + 2, 1)

        for g in range(n // 2 + 2):
            near = a1[3 + g, pl.ds(0, m // 2 + 2)]
            far = a1[3 + g, pl.ds(m // 2 + 6, 2)]
            for e in range(2):
                w0[g, pl.ds(e, m // 2 + 2, stride=2)] = near
                w0[g, pl.ds(m + 4 + e, 2, stride=2)] = far
        for g in range(n // 2 + 2):
            add = jnp.concatenate([w0[g], w0[g]], axis=1)
            for e in range(2):
                a0[2 + 2 * g + e] = a0[2 + 2 * g + e] + add
        smooth(a0, b0, f0, co[11], 3, n + 2, 1)

        smooth(b0, a0, f0, co[11], 4, 4, 1)
        smooth(b0, a0, f0, co[11], n, 4, 1)

        @pl.when(v < SWEEPS * VCYCLES - 1)
        def _():
            for copy in plane_faces():
                copy.start()

        for h in range(2):
            smooth(b0, a0, f0, co[11], 8 + h * (n // 2 - 4), n // 2 - 4, 1)

            @pl.when(v < SWEEPS * VCYCLES - 1)
            def _():
                for copy in row_faces(h):
                    copy.start()

    def plane_faces():
        return exchange(
            0, a0, la, 4, n, m, m + 8, 4, 4, [(a, b) for a in (-1, 1) for b in (-1, 0, 1)], start=False
        )

    def row_faces(h):
        ps = pl.ds(4 + h * (n // 2), n // 2)
        faces = []
        for i, b in enumerate((-1, 1)):
            qs, qd = span(b, m, 0, m + 4, 4)
            faces.append(remote(a0.at[ps, qs], la.at[ps, qd], side_s.at[i, h], side_r.at[i, h], at(dz=b)))
        return faces

    def land_rows(h):
        for copy in row_faces(h):
            copy.wait_recv()
        for k in range(n // 2):
            p = 4 + h * (n // 2) + k
            a0[p, pl.ds(m, 8)] = la[p, pl.ds(m, 8)]

    def land_planes():
        for copy in plane_faces():
            copy.wait_recv()
        for p in list(range(4)) + list(range(n + 4, n + 8)):
            a0[p] = la[p]

    def all_sent():
        for copy in plane_faces() + row_faces(0) + row_faces(1):
            copy.wait_send()

    def turn(v, _):
        @pl.when(lax.rem(v, VCYCLES) == 0)
        def _():
            @pl.when(v > 0)
            def _():
                land_rows(0)
                land_rows(1)
                land_planes()
                second_right()
                all_sent()

            smooth(a0, b0, f0, co[11], 1, n + 6, 2)

        @pl.when(lax.rem(v, VCYCLES) != 0)
        def _():
            land_rows(0)
            smooth(a0, b0, f0, co[11], 5, n // 2 - 2, 1)
            land_rows(1)
            smooth(a0, b0, f0, co[11], n // 2 + 3, n // 2, 1)
            land_planes()
            smooth(a0, b0, f0, co[11], 1, 4, 1)
            smooth(a0, b0, f0, co[11], n + 3, 4, 1)
            all_sent()

        cycle(v)
        return 0

    lax.fori_loop(0, SWEEPS * VCYCLES, turn, 0)

    def sent(d):
        src = ready.at[d]
        dst = out.at[:, pl.ds(pl.multiple_of(z * m, m), m), :]
        if d == 0:
            return pltpu.make_async_copy(src, dst, out_s.at[0])
        return remote(src, dst, out_s.at[d], out_r.at[d], at(dz=d))

    for d in (4, 3, 5, 2, 6, 1, 7, 0):
        first = 4 + 4 * lax.rem(z + d, NZ)
        block = a0[pl.ds(first, 4), pl.ds(0, m)].reshape(4 * m, 2 * half)
        ready[d] = choose(block, joined[...]).reshape(4, m, 2 * half)
        sent(d).start()
    for d in (1, 7, 2, 6, 3, 5, 4):
        sent(d).wait_recv()
    for d in range(1, NZ):
        sent(d).wait_send()
    sent(0).wait()


def per_device(initial, kappa):
    count = lax.axis_size("node")
    assert count == 2 * NX and lax.axis_size("space") == NY * NZ
    thick, rows, cols = initial.shape
    assert thick == 4 and rows == 256 and cols == 256
    n, m = thick * NZ, rows // NZ
    f32 = jnp.float32
    full = pltpu.VMEM((n + 8, m + 8, cols), f32)
    mid = pltpu.VMEM((n // 2 + 8, m // 2 + 8, cols // 2), f32)
    low = pltpu.VMEM((n // 4 + 16, m // 4 + 16, cols // 2), f32)
    dma = pltpu.SemaphoreType.DMA
    chunks = pltpu.VMEM((8, n // 8, m, cols), f32)
    pick = lambda i, j: pltpu.VMEM((i, j), jnp.bfloat16)
    hbm = pl.BlockSpec(memory_space=pl.ANY)
    result = pl.pallas_call(
        kernel,
        out_shape=pltpu.VMEM((thick, rows, cols), f32),
        in_specs=[hbm, hbm, hbm],
        out_specs=pl.BlockSpec(memory_space=pltpu.VMEM),
        scratch_shapes=[
            pltpu.SMEM((count * ROW,), f32),
            pltpu.VMEM((2, n + 8, m + 8, cols), f32), full, full, full, full,
            pltpu.VMEM((2, 2, 8, n // 8, m, cols), f32), chunks, chunks, chunks,
            pltpu.VMEM((n // 2, m, cols // 2), f32), pltpu.VMEM((n // 2 + 2, m + 8, cols // 2), f32),
            mid, mid, mid,
            pltpu.VMEM((n // 4, m // 2, cols // 2), f32), pltpu.VMEM((n // 4, m // 4, cols // 2), f32),
            pltpu.VMEM((n // 4, m // 2, cols // 2), f32),
            pltpu.VMEM((n // 8 + 8, m // 4 + 16, cols // 2), f32), low, low, low,
            pick(cols, cols), pick(cols, cols), pick(cols // 2, cols // 2), pick(cols // 2, cols // 2),
            dma((NZ,)), dma((NZ,)), dma((8, NZ)), dma((8, NZ)), dma((5, 8)), dma((5, 8)), dma((2, 8)), dma((2, 8)), dma((2, 2)), dma((2, 2)),
            dma((NZ,)), dma((NZ,)), dma((1,)),
        ],
        compiler_params=pltpu.CompilerParams(collective_id=0, has_side_effects=True, vmem_limit_bytes=60 * 2**20),
    )(jnp.asarray(coefficients(count)), initial, kappa)
    return result[None]


def solution(mesh):
    slab = P("space", None, None)
    return jax.shard_map(
        per_device, mesh=mesh, in_specs=(slab, slab), out_specs=P("node", "space", None, None), check_vma=False
    )
```
